32 devices in a mesh: seq: 8 (over y, x, core), tp: 4 (over z).
Axes of the slice: x: 2, y: 2, z: 4, core: 2. Of those that a mesh axis runs over, the one named last changes fastest.
Arguments:
- tokens: bfloat16 [4096, 3584], P('seq'), may hold values from -6 to 6
- norm_gain: float32 [3584], replicated, may hold values from 0.5 to 1.5
- q_weight: bfloat16 [3584, 3584], P(None, 'tp'), may hold values from -0.09375 to 0.09375
- q_bias: float32 [3584], P('tp'), may hold values from -9 to 9
- k_weight: bfloat16 [3584, 512], P(None, 'tp'), may hold values from -0.09375 to 0.09375
- k_bias: float32 [512], P('tp'), may hold values from -9 to 9
- v_weight: bfloat16 [3584, 512], P(None, 'tp'), may hold values from -0.09375 to 0.09375
- v_bias: float32 [512], P('tp'), may hold values from -5 to 5
- o_weight: bfloat16 [3584, 3584], P('tp'), may hold values from -0.09375 to 0.09375
- doc_ids: int32 [4096], replicated, may hold values from 0 to 7, never falling along the last dimension, each value on 1 to 2560 neighbouring positions
Outputs:
- attn_out: bfloat16 [4096, 3584], P('seq', 'tp')
The draws below stay inside these ranges and needn't reach their ends.
Inputs may be any that keep to these rules, and one draw needn't show every extreme that they name: `doc_ids`: document numbers never fall along the sequence; each document holds 1 to 2560 tokens and one holds exactly that many.
All inputs are finite; a program needn't handle non-finite values.
Results may differ from the reference program's by a relative error of at most 0.012.
Values may be sent and summed in bfloat16 or wider, within the bound.
A program may use at most 128 MiB of HBM per device.

```python
import math
import jax
import jax.numpy as jnp
import numpy as np
from jax import lax

D = 3584
HQ = 28
KVH = 4
HD = 128
TOK_DEV = 512
DOCS = 8
TOKENS = 4096
N_TP = 4


def bias_noise(key, count):
    return jnp.clip(jax.random.normal(key, (count,), jnp.float32), -5.0, 5.0)


def bias_plan(key):
    base = jax.random.fold_in(key, 9157)
    signs = (jax.random.randint(jax.random.fold_in(base, 1), (HD,), 0, 2) * 2 - 1).astype(jnp.float32)
    across = jnp.arange(HD) % (HD // 2)
    pattern = jnp.where(across >= HD // 2 - HD // 8, signs, 0.0)
    strong = jax.random.randint(jax.random.fold_in(base, 2), (), 0, KVH)
    order = jax.random.permutation(jax.random.fold_in(base, 3), HQ // KVH)
    levels = [115.0, -105.0, 60.0, 30.0]
    tops = jnp.concatenate([jnp.array(levels, jnp.float32), jnp.zeros((HQ // KVH - 4,), jnp.float32)])
    strength = tops[order]
    key_level = math.sqrt(4.0 * levels[0] / math.sqrt(HD))
    return (pattern, strong, strength, key_level)


def draw_k_bias(key, part):
    pattern, strong, strength, key_level = bias_plan(key)
    noise = bias_noise(jax.random.fold_in(key, 31), KVH * HD).reshape(KVH, HD)
    chosen = (jnp.arange(KVH) == strong)[:, None] & (pattern != 0.0)[None, :]
    return jnp.where(chosen, key_level * pattern[None, :], noise).reshape(KVH * HD).astype(jnp.float32)


def draw_q_bias(key, part):
    pattern, strong, strength, key_level = bias_plan(key)
    group = HQ // KVH
    noise = bias_noise(jax.random.fold_in(key, 37), HQ * HD).reshape(KVH, group, HD)
    level = 4.0 * strength / (math.sqrt(HD) * key_level)
    chosen = (jnp.arange(KVH) == strong)[:, None, None] & (strength != 0.0)[None, :, None] & (pattern != 0.0)[None, None, :]
    aligned = level[None, :, None] * pattern[None, None, :]
    return jnp.where(chosen, aligned, noise).reshape(HQ * HD).astype(jnp.float32)


def shard_levels(stream_key, extent, split, smallest, top_value):
    gain = 1.0
    for dim, shards_of in split:
        draws = jax.random.uniform(jax.random.fold_in(jax.random.fold_in(stream_key, 6), dim), (shards_of,), jnp.float32, smallest / len(split), top_value / len(split))
        gain = gain * jnp.repeat(jnp.exp(draws), extent[dim] // shards_of).reshape((-1,) + (1,) * (len(extent) - 1 - dim))
    return gain


def length_profile(amount, total, most, skew):
    portions = [(1 << 20) // math.isqrt(standing ** skew) + 1 for standing in range(2, amount + 1)]
    rest, given = total - most - (amount - 1), [1] * (amount - 1)
    while rest > 0:
        movable = [i for i in range(amount - 1) if given[i] < most]
        pool, left = sum([portions[i] for i in movable]), rest
        for i in movable:
            addition = min(most - given[i], max(1, left * portions[i] // pool), rest)
            given[i] = given[i] + addition
            rest = rest - addition
    return np.array([most] + given)


def uneven_parts(stream_key, amount, total, most, lean):
    if amount == 2:
        one = jax.random.randint(stream_key, (), max(1, total - most), min(most, total - 1) + 1)
        return jnp.stack([one, total - one])
    lengths = jnp.asarray(length_profile(amount, total, most, lean), jnp.int32)
    twos = (amount - 1) // 2
    giver, taker = lengths[1:1 + 2 * twos:2], lengths[2:2 + 2 * twos:2]
    slack = jnp.minimum(giver - 1, most - taker)
    moved = jax.random.randint(jax.random.fold_in(stream_key, 1), (twos,), 0, 1 << 20) % (slack + 1)
    lengths = lengths.at[1:1 + 2 * twos:2].set(giver - moved).at[2:2 + 2 * twos:2].set(taker + moved)
    return lengths[jax.random.permutation(jax.random.fold_in(stream_key, 2), amount)]


def normal_values(own_key, shape, scale, reach, split=(), held_as=jnp.bfloat16):
    values = jax.random.normal(own_key, shape, jnp.float32) * scale
    if len(split) > 0:
        values = shard_levels(own_key, shape, split, -0.22, 0.18) * values
    return jnp.clip(values, min=-reach, max=reach).astype(held_as)


def setup_inputs(seed: int = 0) -> dict:
    key_list = jax.random.split(jax.random.key(seed), 11)
    tokens = normal_values(key_list[0], (TOKENS, D), 1.0, 6.0, ((0, 8),))
    norm_gain = jnp.clip(1.0 + 0.1 * jax.random.normal(key_list[1], (D,), jnp.float32), 0.5, 1.5)
    q_weight = normal_values(key_list[2], (D, HQ * HD), D ** -0.5, 0.09375, ((1, 4),))
    q_bias = draw_q_bias(jax.random.fold_in(key_list[10], 71), 0)
    k_weight = normal_values(key_list[4], (D, KVH * HD), D ** -0.5, 0.09375, ((1, 4),))
    k_bias = draw_k_bias(jax.random.fold_in(key_list[10], 71), 0)
    v_weight = normal_values(key_list[6], (D, KVH * HD), D ** -0.5, 0.09375, ((1, 4),))
    v_bias = normal_values(key_list[7], (KVH * HD,), 1.0, 5.0, ((0, 4),), jnp.float32)
    o_weight = normal_values(key_list[8], (HQ * HD, D), (HQ * HD) ** -0.5, 0.09375, ((0, 4),))
    doc_ids = jnp.searchsorted(jnp.cumsum(uneven_parts(key_list[9], DOCS, TOKENS, TOKENS // 2 + TOK_DEV, 0)), jnp.arange(TOKENS), side="right").astype(jnp.int32)
    return {"tokens": tokens, "norm_gain": norm_gain, "q_weight": q_weight, "q_bias": q_bias, "k_weight": k_weight, "k_bias": k_bias, "v_weight": v_weight, "v_bias": v_bias, "o_weight": o_weight, "doc_ids": doc_ids}


rope_base = 1000000.0

def rotate(t, posf):
    half = t.shape[-1] // 2
    inv = rope_base ** (-(jnp.arange(half, dtype=jnp.float32) * 2.0) / t.shape[-1])
    angle = posf[:, None] * inv[None, :]
    angle = jnp.concatenate([angle, angle], axis=-1)
    turned = jnp.concatenate([-t[..., half:], t[..., :half]], axis=-1)
    return t * jnp.cos(angle)[:, None, :] + turned * jnp.sin(angle)[:, None, :]

def reference(tokens, norm_gain, q_weight, q_bias, k_weight, k_bias, v_weight, v_bias, o_weight, doc_ids):
    widened = tokens.astype(jnp.float32)
    normed = (widened * lax.rsqrt(lax.optimization_barrier(jnp.mean(widened * widened, axis=-1, keepdims=True)) + 1e-06) * norm_gain).astype(jnp.bfloat16)
    posf = jnp.arange(TOKENS).astype(jnp.float32)
    group = HQ // KVH
    query = jnp.dot(normed, q_weight, preferred_element_type=jnp.float32) + q_bias
    query = rotate(query.reshape(TOKENS, HQ, HD), posf).astype(jnp.bfloat16).reshape(TOKENS, KVH, group, HD)
    keys = jnp.dot(normed, k_weight, preferred_element_type=jnp.float32) + k_bias
    keys = rotate(keys.reshape(TOKENS, KVH, HD), posf).astype(jnp.bfloat16)
    values = (jnp.dot(normed, v_weight, preferred_element_type=jnp.float32) + v_bias).astype(jnp.bfloat16).reshape(TOKENS, KVH, HD)
    block = min(512, TOKENS)
    scale = 1.0 / HD ** 0.5
    kpos = jnp.arange(TOKENS).astype(jnp.int32)
    keys_f = keys.astype(jnp.float32)
    values_f = values.astype(jnp.float32)

    def attend(index):
        first = (index * block).astype(jnp.int32)
        qblock = lax.dynamic_slice_in_dim(query, first, block, 0).astype(jnp.float32)
        qdoc = lax.dynamic_slice_in_dim(doc_ids, first, block, 0)
        qpos = first + jnp.arange(block).astype(jnp.int32)
        scores = jnp.einsum('qkgd,tkd->kgqt', qblock, keys_f) * scale
        visible = (kpos[None, :] <= qpos[:, None]) & (qdoc[:, None] == doc_ids[None, :])
        scores = jnp.where(visible, scores, -1e+30)
        top = lax.optimization_barrier(jnp.max(scores, axis=-1, keepdims=True))
        expd = jnp.where(visible, jnp.exp(scores - top), 0.0)
        total = lax.optimization_barrier(jnp.sum(expd, axis=-1))
        weights = expd.astype(jnp.bfloat16).astype(jnp.float32)
        summed = jnp.einsum('kgqt,tkd->kgqd', weights, values_f) / total[..., None]
        return jnp.transpose(summed, (2, 0, 1, 3)).astype(jnp.bfloat16).reshape(block, HQ * HD)
    context = lax.map(attend, jnp.arange(TOKENS // block)).reshape(TOKENS, HQ * HD)
    width = HQ * HD // N_TP
    result = jnp.zeros((TOKENS, D), jnp.float32)
    for index in range(N_TP):
        term = jnp.dot(context[:, index * width:(index + 1) * width], o_weight[index * width:(index + 1) * width], preferred_element_type=jnp.float32)
        result = result + term.astype(jnp.bfloat16).astype(jnp.float32)
    return result.astype(jnp.bfloat16)
```

```python
import functools
import math

import jax
import jax.numpy as jnp
import numpy as np
from jax import lax
from jax.experimental import pallas as pl
from jax.experimental.pallas import tpu as pltpu
from jax.sharding import PartitionSpec as P

HD = 128
MESH = pl.DeviceIdType.MESH
rope_base = 1000000.0
VMEM = pltpu.VMEM
LAG = 1
AHEAD = 3
BACK = 1


def rope_tables(rows, blocks):
    half = HD // 2
    inv = rope_base ** (-(np.arange(half, dtype=np.float64) * 2.0) / HD)
    inv = np.concatenate([inv, inv])[None, :]
    near = np.arange(rows)[:, None] * inv
    far = np.arange(blocks)[:, None] * rows * inv
    near = np.stack([np.cos(near), np.sin(near)]).astype(np.float32)
    far = np.stack([np.cos(far), np.sin(far)])[:, :, None, :].astype(np.float32)
    return near, far


def attend(
    seq_count, tp_count, reach, chunk,
    tokens_hbm, gain_ref, wq_hbm, qb_ref, wk_hbm, kb_ref, wv_hbm, vb_ref, wo_hbm,
    kdoc_ref, near_hbm, far_ref, out_ref,
    tokens, normed, wq, wkv, wo, near, q_ref, kv_ref, kv_in, kext, acc, tops, totals, sent, got,
    load_sems, kv_send, kv_pass, kv_recv, send_sem, recv_sem,
):
    place = lax.axis_index("seq")
    turn = lax.axis_index("tp")
    rows, width = tokens.shape[0], wq.shape[1]
    heads = width // HD
    cols = out_ref.shape[1]
    parts = rows // chunk
    factor = math.log2(math.e) / HD**0.5
    step = 2 * HD
    spans = [(lo, min(step, width - lo)) for lo in range(0, width, step)]
    slab = rows // 4
    token_loads = [
        pltpu.make_async_copy(
            tokens_hbm.at[pl.ds(index * slab, slab)], tokens.at[pl.ds(index * slab, slab)],
            load_sems.at[index],
        )
        for index in range(4)
    ]
    near_load = pltpu.make_async_copy(near_hbm, near, load_sems.at[4])
    kv_loads = [
        pltpu.make_async_copy(wk_hbm, wkv.at[:, pl.ds(0, HD)], load_sems.at[5]),
        pltpu.make_async_copy(wv_hbm, wkv.at[:, pl.ds(HD, HD)], load_sems.at[6]),
    ]
    q_loads = [
        pltpu.make_async_copy(
            wq_hbm.at[:, pl.ds(lo, size)], wq.at[:, pl.ds(lo, size)], load_sems.at[7 + index]
        )
        for index, (lo, size) in enumerate(spans)
    ]
    load = pltpu.make_async_copy(wo_hbm, wo, load_sems.at[7 + len(spans)])
    for copy in token_loads + kv_loads + [near_load]:
        copy.start()

    barrier = pltpu.get_barrier_semaphore()
    span = min(reach + 1, seq_count - 1)
    for away in range(1, span + 1):
        @pl.when(place >= away)
        def _():
            pl.semaphore_signal(barrier, inc=1, device_id={"seq": place - away}, device_id_type=MESH)

        @pl.when(place + away < seq_count)
        def _():
            pl.semaphore_signal(barrier, inc=1, device_id={"seq": place + away}, device_id_type=MESH)

    @pl.when(turn > 0)
    def _():
        pl.semaphore_signal(barrier, inc=1, device_id={"tp": turn - 1}, device_id_type=MESH)

    @pl.when(turn < tp_count - 1)
    def _():
        pl.semaphore_signal(barrier, inc=1, device_id={"tp": turn + 1}, device_id_type=MESH)

    behind = jnp.minimum(place, reach)
    near_count = jnp.minimum(place, span) + jnp.minimum(seq_count - 1 - place, span)
    sides = jnp.where(turn > 0, 1, 0) + jnp.where(turn < tp_count - 1, 1, 0)

    lane = lax.broadcasted_iota(jnp.int32, (rows, HD), 1)
    doc = lax.broadcasted_iota(jnp.int32, (HD, rows), 0)
    for away in range(reach + 1):
        ids = kdoc_ref[jnp.maximum(place - away, 0)]
        kext[away] = jnp.where(doc == ids, 1.0, 0.0).T.astype(jnp.bfloat16)
        if away == 0:
            veto = jnp.where(doc == ids, 0.0, -1e30).astype(jnp.bfloat16)
            for part in range(parts):
                q_ref[part, HD:, :] = jnp.concatenate([veto[:, part * chunk:(part + 1) * chunk]] * heads, axis=1)

    gain = gain_ref[...].reshape(1, gain_ref.shape[0])
    for index in range(4):
        token_loads[index].wait()
        if index == 3:
            for copy in q_loads:
                copy.start()

        @pl.loop(0, slab // 64)
        def _(step):
            cut = pl.ds(pl.multiple_of(index * slab + step * 64, 64), 64)
            wide = tokens[cut, :].astype(jnp.float32)
            mean = jnp.mean(wide * wide, axis=-1, keepdims=True)
            normed[cut, :] = (wide * lax.rsqrt(mean + 1e-06) * gain).astype(jnp.bfloat16)

    near_load.wait()
    far_cos, far_sin = far_ref[0, place], far_ref[1, place]
    cos = near[0] * far_cos - near[1] * far_sin
    sin = near[1] * far_cos + near[0] * far_sin
    near[0] = cos
    near[1] = jnp.where(lane < HD // 2, -sin, sin)

    def rope(t):
        return t * near[0] + pltpu.roll(t, HD // 2, 1) * near[1]

    for copy in kv_loads:
        copy.wait()
    kv = jnp.dot(normed[...], wkv[...], preferred_element_type=jnp.float32)
    kv_ref[0] = rope(kv[:, :HD] + kb_ref[...].reshape(1, HD)).astype(jnp.bfloat16)
    values = kv[:, HD:] + vb_ref[...].reshape(1, HD)
    for lo in range(0, rows, HD):
        kv_ref[1, lo:lo + HD] = values[lo:lo + HD].T.astype(jnp.bfloat16)

    pl.semaphore_wait(barrier, near_count + sides)

    odd = lax.rem(place, 2) == 1
    partner = place + 1 - 2 * lax.rem(place, 2)

    def kv_copy(away):
        return pltpu.make_async_remote_copy(
            src_ref=kv_ref, dst_ref=kv_in.at[away - 1],
            send_sem=kv_send.at[away - 1], recv_sem=kv_recv.at[away - 1],
            device_id={"seq": lax.rem(place + away, seq_count)}, device_id_type=MESH,
        )

    def relay(away, landing):
        return pltpu.make_async_remote_copy(
            src_ref=kv_in.at[away - 1], dst_ref=kv_in.at[landing - 1],
            send_sem=kv_pass.at[away - 1], recv_sem=kv_recv.at[landing - 1],
            device_id={"seq": partner}, device_id_type=MESH,
        )

    evens = [away for away in range(2, reach + 2, 2) if away < seq_count]

    def wanted(away):
        return odd if away > reach else (place >= 0)

    def each_send(act):
        for away in evens:
            @pl.when((place + away < seq_count) & wanted(away))
            def _():
                act(kv_copy(away))

        @pl.when(jnp.logical_not(odd))
        def _():
            act(kv_copy(1))

    def each_relay(act):
        for away in evens:
            if away + 1 <= reach:
                @pl.when((place >= away) & jnp.logical_not(odd))
                def _():
                    act(relay(away, away + 1))

            @pl.when((place >= away) & odd)
            def _():
                act(relay(away, away - 1))

    each_send(lambda copy: copy.start())

    for index, (lo, size) in enumerate(spans):
        q_loads[index].wait()
        if index == 1:
            load.start()
        out = jnp.dot(
            normed[...], wq[:, lo:lo + size], preferred_element_type=jnp.float32
        ) + qb_ref[lo:lo + size].reshape(1, size)
        for head in range(0, size, HD):
            turned = rope(out[:, head:head + HD]) * factor
            at = (lo + head) // HD * chunk
            for part in range(parts):
                q_ref[part, :HD, at:at + chunk] = turned[part * chunk:(part + 1) * chunk].T.astype(jnp.bfloat16)

    for away in evens:
        @pl.when((place >= away) & wanted(away))
        def _():
            kv_copy(away).wait_recv()

        if away + 1 <= reach:
            @pl.when((place >= away) & jnp.logical_not(odd))
            def _():
                relay(away, away + 1).start()

        @pl.when((place >= away) & odd)
        def _():
            relay(away, away - 1).start()

    def term_copy(side, dest, part):
        cut = pl.ds(pl.multiple_of(part * chunk, chunk), chunk)
        target = lax.rem(turn + (1 if side == 0 else tp_count - 1), tp_count)
        return pltpu.make_async_remote_copy(
            src_ref=sent.at[dest, cut], dst_ref=got.at[side, dest, cut],
            send_sem=send_sem.at[dest, part], recv_sem=recv_sem.at[side, dest, part],
            device_id={"tp": target}, device_id_type=MESH,
        )

    order = sorted(range(tp_count), key=lambda d: (-abs(2 * d - tp_count + 1), -d))

    def forward(part, first):
        cut = pl.ds(pl.multiple_of(part * chunk, chunk), chunk)
        for side in (0, 1):
            chosen = (2 * turn < tp_count) if (side == 0) == first else (2 * turn >= tp_count)
            for dest in order:
                inner = (turn > 0) & (dest > turn) if side == 0 else (
                    (turn < tp_count - 1) & (dest < turn))

                @pl.when(inner & chosen)
                def _():
                    term_copy(side, dest, part).wait_recv()
                    sent[dest, cut] = (
                        sent[dest, cut].astype(jnp.float32) + got[side, dest, cut].astype(jnp.float32)
                    ).astype(jnp.bfloat16)
                    term_copy(side, dest, part).start()

    def finish(part):
        cut = pl.ds(pl.multiple_of(part * chunk, chunk), chunk)
        for dest in range(tp_count):
            for side in (0, 1):
                edge = (turn > 0) if side == 0 else (turn < tp_count - 1)

                @pl.when((dest == turn) & edge)
                def _():
                    term_copy(side, dest, part).wait_recv()

            @pl.when(dest == turn)
            def _():
                total = sent[dest, cut].astype(jnp.float32)
                left = jnp.where(turn > 0, got[0, dest, cut].astype(jnp.float32), 0.0)
                right = jnp.where(turn < tp_count - 1, got[1, dest, cut].astype(jnp.float32), 0.0)
                out_ref[cut, :] = (total + left + right).astype(jnp.bfloat16)

    wide = step // chunk * chunk
    tiles = [(lo, min(wide, heads * chunk - lo)) for lo in range(0, heads * chunk, wide)]

    def piece(part):
        cut = pl.ds(pl.multiple_of(part * chunk, chunk), chunk)
        def block(held, away, first):
            keys = jnp.concatenate([held[0], kext[away]], axis=1)
            values = jnp.concatenate([held[1, lo:lo + HD] for lo in range(0, rows, HD)], axis=1)
            if first:
                key = lax.broadcasted_iota(jnp.int32, (rows, chunk), 0)
                row = part * chunk + lax.broadcasted_iota(jnp.int32, (rows, chunk), 1)
                later = jnp.where(key <= row, 0.0, -1e30)
            def score(tile):
                lo, size = tile
                s = jnp.dot(keys, q_ref[part, :, lo:lo + size], preferred_element_type=jnp.float32)
                if first:
                    s = s + jnp.concatenate([later] * (size // chunk), axis=1)
                return s

            def weigh(tile, s):
                lo, size = tile
                fresh = jnp.max(s, axis=0, keepdims=True)
                scale = None
                if not first:
                    top = tops[:, lo:lo + size]
                    fresh = jnp.maximum(top, fresh)
                    scale = jnp.exp2(top - fresh)
                e = jnp.exp2(s - fresh)
                total = jnp.sum(e, axis=0, keepdims=True)
                if not first:
                    total = total + totals[:, lo:lo + size] * scale
                tops[:, lo:lo + size] = fresh
                totals[:, lo:lo + size] = total
                return tile, scale, e.astype(jnp.bfloat16)

            def mix(tile, scale, e):
                return tile, scale, jnp.dot(values, e, preferred_element_type=jnp.float32)

            def gather(tile, scale, pv):
                lo, size = tile
                if not first:
                    pv = pv + acc[:, lo:lo + size] * scale
                acc[:, lo:lo + size] = pv

            ready = [score(tile) for tile in tiles[:AHEAD]]
            mixed = []
            for index, tile in enumerate(tiles):
                if index + AHEAD < len(tiles):
                    ready.append(score(tiles[index + AHEAD]))
                mixed.append(mix(*weigh(tile, ready.pop(0))))
                if len(mixed) > BACK:
                    gather(*mixed.pop(0))
            while mixed:
                gather(*mixed.pop(0))

        block(kv_ref, 0, True)

        @pl.loop(1, behind + 1)
        def _(away):
            @pl.when((part == 0) & (lax.rem(away, 2) == 1))
            def _():
                kv_copy(away).wait_recv()

            block(kv_in.at[away - 1], away, False)

        whole = acc[...] * (1.0 / totals[...])
        context = jnp.concatenate(
            [whole[:, h * chunk:(h + 1) * chunk].T.astype(jnp.bfloat16) for h in range(heads)], axis=1
        )

        @pl.when(part == 0)
        def _():
            load.wait()

        for dest in order:
            sent[dest, cut] = jnp.dot(
                context, wo[:, dest * cols:(dest + 1) * cols], preferred_element_type=jnp.float32
            ).astype(jnp.bfloat16)
        for dest in order:
            @pl.when((turn == 0) & (dest > 0))
            def _():
                term_copy(0, dest, part).start()

            @pl.when((turn == tp_count - 1) & (dest < tp_count - 1))
            def _():
                term_copy(1, dest, part).start()

    @pl.loop(0, parts + LAG + 1)
    def _(part):
        @pl.when(part < parts)
        def _():
            piece(part)

        @pl.when((part >= LAG) & (part < parts + LAG))
        def _():
            forward(part - LAG, True)

        @pl.when(part >= LAG + 1)
        def _():
            forward(part - LAG - 1, False)

    @pl.loop(0, parts)
    def _(part):
        finish(part)

    @pl.loop(0, parts)
    def _(part):
        for dest in range(tp_count):
            @pl.when(dest != turn)
            def _():
                term_copy(0, dest, part).wait_send()

    each_send(lambda copy: copy.wait_send())
    each_relay(lambda copy: copy.wait_send())


def body(
    tokens, norm_gain, q_weight, q_bias, k_weight, k_bias, v_weight, v_bias, o_weight, doc_ids
):
    rows, model = tokens.shape
    seq_count = lax.axis_size("seq")
    tp_count = lax.axis_size("tp")
    width = q_weight.shape[1]
    cols = o_weight.shape[1] // tp_count
    reach = min(seq_count - 1, (seq_count * rows // 2 + 2 * rows - 2) // rows)
    chunk = rows // 2
    parts = rows // chunk
    near, far = rope_tables(rows, seq_count)
    hbm = pl.BlockSpec(memory_space=pl.ANY)
    vmem = pl.BlockSpec(memory_space=VMEM)
    slots = reach + 1
    spans = -(-width // (2 * HD))
    kdoc = doc_ids.reshape(seq_count, 1, rows)
    return pl.pallas_call(
        functools.partial(attend, seq_count, tp_count, reach, chunk),
        out_shape=jax.ShapeDtypeStruct((rows, cols), jnp.bfloat16),
        in_specs=[hbm, vmem, hbm, vmem, hbm, vmem, hbm, vmem, hbm, vmem, hbm, vmem],
        out_specs=vmem,
        scratch_shapes=[
            VMEM((rows, model), jnp.bfloat16),
            VMEM((rows, model), jnp.bfloat16),
            VMEM((model, width), jnp.bfloat16),
            VMEM((model, 2 * HD), jnp.bfloat16),
            VMEM(o_weight.shape, jnp.bfloat16),
            VMEM((2, rows, HD), jnp.float32),
            VMEM((parts, 2 * HD, width // HD * chunk), jnp.bfloat16),
            VMEM((2, rows, HD), jnp.bfloat16),
            VMEM((slots, 2, rows, HD), jnp.bfloat16),
            VMEM((slots, rows, HD), jnp.bfloat16),
            VMEM((HD, width // HD * chunk), jnp.float32),
            VMEM((1, width // HD * chunk), jnp.float32),
            VMEM((1, width // HD * chunk), jnp.float32),
            VMEM((tp_count, rows, cols), jnp.bfloat16),
            VMEM((2, tp_count, rows, cols), jnp.bfloat16),
            pltpu.SemaphoreType.DMA((8 + spans,)),
            pltpu.SemaphoreType.DMA((slots,)),
            pltpu.SemaphoreType.DMA((slots,)),
            pltpu.SemaphoreType.DMA((slots,)),
            pltpu.SemaphoreType.DMA((tp_count, parts)),
            pltpu.SemaphoreType.DMA((2, tp_count, parts)),
        ],
        compiler_params=pltpu.CompilerParams(
            collective_id=0, has_side_effects=True, vmem_limit_bytes=56 * 1024 * 1024
        ),
    )(
        tokens, norm_gain, q_weight, q_bias, k_weight, k_bias, v_weight, v_bias, o_weight,
        kdoc, jnp.asarray(near), jnp.asarray(far),
    )


def solution(mesh):
    placed = (
        P("seq", None),
        P(),
        P(None, "tp"),
        P("tp"),
        P(None, "tp"),
        P("tp"),
        P(None, "tp"),
        P("tp"),
        P("tp", None),
        P(),
    )
    return jax.shard_map(
        body, mesh=mesh, in_specs=placed, out_specs=P("seq", "tp"), check_vma=False
    )
```

```python
import functools
import math

import jax
import jax.numpy as jnp
import numpy as np
from jax import lax
from jax.experimental import pallas as pl
from jax.experimental.pallas import tpu as pltpu
from jax.sharding import PartitionSpec as P

HD = 128
MESH = pl.DeviceIdType.MESH
rope_base = 1000000.0
VMEM = pltpu.VMEM
SUBS = 2
AHEAD = 3
BACK = 1


def rope_tables(rows, blocks):
    half = HD // 2
    inv = rope_base ** (-(np.arange(half, dtype=np.float64) * 2.0) / HD)
    inv = np.concatenate([inv, inv])[None, :]
    near = np.arange(rows)[:, None] * inv
    far = np.arange(blocks)[:, None] * rows * inv
    near = np.stack([np.cos(near), np.sin(near)]).astype(np.float32)
    far = np.stack([np.cos(far), np.sin(far)])[:, :, None, :].astype(np.float32)
    return near, far


def attend(
    seq_count, tp_count, reach, chunk, team,
    tokens_hbm, gain_ref, wq_hbm, qb_ref, wk_hbm, kb_ref, wv_hbm, vb_ref, wo_hbm,
    kdoc_ref, near_hbm, far_ref, out_ref,
    tokens, normed, wq, wkv, wo, near, q_ref, kv_ref, kv_in, kext, acc, tops, totals, ctx, ctx_in, lent, sent, got,
    load_sems, kv_send, kv_pass, kv_recv, send_sem, recv_sem, ctx_send, ctx_recv, lent_send, lent_recv,
):
    place = lax.axis_index("seq")
    turn = lax.axis_index("tp")
    rows, width = tokens.shape[0], wq.shape[1]
    heads = width // HD
    cols = out_ref.shape[1]
    parts = rows // chunk
    factor = math.log2(math.e) / HD**0.5
    step = 2 * HD
    spans = [(lo, min(step, width - lo)) for lo in range(0, width, step)]
    slab = rows // 4
    token_loads = [
        pltpu.make_async_copy(
            tokens_hbm.at[pl.ds(index * slab, slab)], tokens.at[pl.ds(index * slab, slab)],
            load_sems.at[index],
        )
        for index in range(4)
    ]
    near_load = pltpu.make_async_copy(near_hbm, near, load_sems.at[4])
    kv_loads = [
        pltpu.make_async_copy(wk_hbm, wkv.at[:, pl.ds(0, HD)], load_sems.at[5]),
        pltpu.make_async_copy(wv_hbm, wkv.at[:, pl.ds(HD, HD)], load_sems.at[6]),
    ]
    q_loads = [
        pltpu.make_async_copy(
            wq_hbm.at[:, pl.ds(lo, size)], wq.at[:, pl.ds(lo, size)], load_sems.at[7 + index]
        )
        for index, (lo, size) in enumerate(spans)
    ]
    load = pltpu.make_async_copy(wo_hbm, wo, load_sems.at[7 + len(spans)])
    for copy in token_loads + kv_loads + [near_load]:
        copy.start()

    barrier = pltpu.get_barrier_semaphore()
    span = min(reach + 1, seq_count - 1)
    for away in range(1, span + 1):
        @pl.when(place >= away)
        def _():
            pl.semaphore_signal(barrier, inc=1, device_id={"seq": place - away}, device_id_type=MESH)

        @pl.when(place + away < seq_count)
        def _():
            pl.semaphore_signal(barrier, inc=1, device_id={"seq": place + away}, device_id_type=MESH)

    @pl.when(turn > 0)
    def _():
        pl.semaphore_signal(barrier, inc=1, device_id={"tp": turn - 1}, device_id_type=MESH)

    @pl.when(turn < tp_count - 1)
    def _():
        pl.semaphore_signal(barrier, inc=1, device_id={"tp": turn + 1}, device_id_type=MESH)

    behind = jnp.minimum(place, reach)
    near_count = jnp.minimum(place, span) + jnp.minimum(seq_count - 1 - place, span)
    sides = jnp.where(turn > 0, 1, 0) + jnp.where(turn < tp_count - 1, 1, 0)

    lane = lax.broadcasted_iota(jnp.int32, (rows, HD), 1)
    doc = lax.broadcasted_iota(jnp.int32, (HD, rows), 0)
    for away in range(reach + 1):
        ids = kdoc_ref[jnp.maximum(place - away, 0)]
        kext[away] = jnp.where(doc == ids, 1.0, 0.0).T.astype(jnp.bfloat16)
        if away == 0:
            veto = jnp.where(doc == ids, 0.0, -1e30).astype(jnp.bfloat16)
            for part in range(parts):
                q_ref[part, HD:, :] = jnp.concatenate([veto[:, part * chunk:(part + 1) * chunk]] * heads, axis=1)

    pl.semaphore_wait(barrier, near_count + sides)
    half = tp_count // 2
    right = turn // half
    inner = (turn > 0) & (turn < tp_count - 1)
    outer = jnp.logical_not(inner)
    share = width // team
    mine = lax.rem(place, team)
    base = place - mine
    partner = place + 1 - 2 * lax.rem(place, 2)
    lent_cols = (tp_count - 1) * cols
    steps = list(range(2, team, 2))

    def lend():
        rows_cut = pl.ds(pl.multiple_of(mine * share, 16), share)
        cols_cut = pl.ds(pl.multiple_of((1 - right) * cols, HD), lent_cols)
        return pltpu.make_async_remote_copy(
            src_ref=wo_hbm.at[rows_cut, cols_cut], dst_ref=lent.at[rows_cut],
            send_sem=lent_send.at[0], recv_sem=lent_recv.at[mine],
            device_id={"tp": turn + 1 - 2 * right}, device_id_type=MESH,
        )

    def spread(piece_of, slot, target):
        rows_cut = pl.ds(pl.multiple_of(piece_of * share, 16), share)
        return pltpu.make_async_remote_copy(
            src_ref=lent.at[rows_cut], dst_ref=lent.at[rows_cut],
            send_sem=lent_send.at[slot], recv_sem=lent_recv.at[piece_of],
            device_id={"seq": target}, device_id_type=MESH,
        )

    def own_spreads():
        return [spread(mine, 1, partner)] + [
            spread(mine, 2 + index, base + lax.rem(mine + away, team))
            for index, away in enumerate(steps)
        ]

    def passed_spreads():
        return [
            spread(lax.rem(mine + team - away, team), 2 + len(steps) + index, partner)
            for index, away in enumerate(steps)
        ]

    @pl.when(outer)
    def _():
        lend().start()

    gain = gain_ref[...].reshape(1, gain_ref.shape[0])
    for index in range(4):
        token_loads[index].wait()
        if index == 3:
            for copy in q_loads:
                copy.start()

        @pl.loop(0, slab // 64)
        def _(step):
            cut = pl.ds(pl.multiple_of(index * slab + step * 64, 64), 64)
            wide = tokens[cut, :].astype(jnp.float32)
            mean = jnp.mean(wide * wide, axis=-1, keepdims=True)
            normed[cut, :] = (wide * lax.rsqrt(mean + 1e-06) * gain).astype(jnp.bfloat16)

    near_load.wait()
    far_cos, far_sin = far_ref[0, place], far_ref[1, place]
    cos = near[0] * far_cos - near[1] * far_sin
    sin = near[1] * far_cos + near[0] * far_sin
    near[0] = cos
    near[1] = jnp.where(lane < HD // 2, -sin, sin)

    def rope(t):
        return t * near[0] + pltpu.roll(t, HD // 2, 1) * near[1]

    for copy in kv_loads:
        copy.wait()
    kv = jnp.dot(normed[...], wkv[...], preferred_element_type=jnp.float32)
    kv_ref[0] = rope(kv[:, :HD] + kb_ref[...].reshape(1, HD)).astype(jnp.bfloat16)
    values = kv[:, HD:] + vb_ref[...].reshape(1, HD)
    for lo in range(0, rows, HD):
        kv_ref[1, lo:lo + HD] = values[lo:lo + HD].T.astype(jnp.bfloat16)

    odd = lax.rem(place, 2) == 1

    def kv_copy(away):
        return pltpu.make_async_remote_copy(
            src_ref=kv_ref, dst_ref=kv_in.at[away - 1],
            send_sem=kv_send.at[away - 1], recv_sem=kv_recv.at[away - 1],
            device_id={"seq": lax.rem(place + away, seq_count)}, device_id_type=MESH,
        )

    def relay(away, landing):
        return pltpu.make_async_remote_copy(
            src_ref=kv_in.at[away - 1], dst_ref=kv_in.at[landing - 1],
            send_sem=kv_pass.at[away - 1], recv_sem=kv_recv.at[landing - 1],
            device_id={"seq": partner}, device_id_type=MESH,
        )

    evens = [away for away in range(2, reach + 2, 2) if away < seq_count]

    def wanted(away):
        return odd if away > reach else (place >= 0)

    def each_send(act):
        for away in evens:
            @pl.when((place + away < seq_count) & wanted(away))
            def _():
                act(kv_copy(away))

        @pl.when(jnp.logical_not(odd))
        def _():
            act(kv_copy(1))

    def each_relay(act):
        for away in evens:
            if away + 1 <= reach:
                @pl.when((place >= away) & jnp.logical_not(odd))
                def _():
                    act(relay(away, away + 1))

            @pl.when((place >= away) & odd)
            def _():
                act(relay(away, away - 1))

    each_send(lambda copy: copy.start())

    for index, (lo, size) in enumerate(spans):
        q_loads[index].wait()
        if index == 1:
            load.start()
        out = jnp.dot(
            normed[...], wq[:, lo:lo + size], preferred_element_type=jnp.float32
        ) + qb_ref[lo:lo + size].reshape(1, size)
        for head in range(0, size, HD):
            turned = rope(out[:, head:head + HD]) * factor
            at = (lo + head) // HD * chunk
            for part in range(parts):
                q_ref[part, :HD, at:at + chunk] = turned[part * chunk:(part + 1) * chunk].T.astype(jnp.bfloat16)

    for away in evens:
        @pl.when((place >= away) & wanted(away))
        def _():
            kv_copy(away).wait_recv()

        if away + 1 <= reach:
            @pl.when((place >= away) & jnp.logical_not(odd))
            def _():
                relay(away, away + 1).start()

        @pl.when((place >= away) & odd)
        def _():
            relay(away, away - 1).start()

    sub = chunk // SUBS

    def sub_cut(index):
        return pl.ds(pl.multiple_of(index * sub, sub), sub)

    def term_copy(side, dest, index):
        return pltpu.make_async_remote_copy(
            src_ref=sent.at[dest, sub_cut(index)], dst_ref=got.at[side, dest, sub_cut(index)],
            send_sem=send_sem.at[dest, index], recv_sem=recv_sem.at[side, dest, index],
            device_id={"tp": turn + 1 - 2 * side}, device_id_type=MESH,
        )

    def ctx_copy(index):
        return pltpu.make_async_remote_copy(
            src_ref=ctx.at[sub_cut(index)], dst_ref=ctx_in.at[sub_cut(index)],
            send_sem=ctx_send.at[index], recv_sem=ctx_recv.at[index],
            device_id={"tp": turn + 1 - 2 * right}, device_id_type=MESH,
        )

    last = tp_count - 1
    far = (1 - right) * last
    home = right * last
    across = last - turn
    farther = (1 - right) * (last - 1) + right
    beside = (1 - right) + right * (last - 1)

    def forward(side, dest, index):
        cut = sub_cut(index)
        term_copy(side, dest, index).wait_recv()
        sent[dest, cut] = (
            sent[dest, cut].astype(jnp.float32) + got[side, dest, cut].astype(jnp.float32)
        ).astype(jnp.bfloat16)
        term_copy(side, dest, index).start()

    wide = step // chunk * chunk
    tiles = [(lo, min(wide, heads * chunk - lo)) for lo in range(0, heads * chunk, wide)]

    def piece(part):
        cut = pl.ds(pl.multiple_of(part * chunk, chunk), chunk)
        def block(held, away, first):
            keys = jnp.concatenate([held[0], kext[away]], axis=1)
            values = jnp.concatenate([held[1, lo:lo + HD] for lo in range(0, rows, HD)], axis=1)
            if first:
                key = lax.broadcasted_iota(jnp.int32, (rows, chunk), 0)
                row = part * chunk + lax.broadcasted_iota(jnp.int32, (rows, chunk), 1)
                later = jnp.where(key <= row, 0.0, -1e30)
            def score(tile):
                lo, size = tile
                s = jnp.dot(keys, q_ref[part, :, lo:lo + size], preferred_element_type=jnp.float32)
                if first:
                    s = s + jnp.concatenate([later] * (size // chunk), axis=1)
                return s

            def weigh(tile, s):
                lo, size = tile
                fresh = jnp.max(s, axis=0, keepdims=True)
                scale = None
                if not first:
                    top = tops[:, lo:lo + size]
                    fresh = jnp.maximum(top, fresh)
                    scale = jnp.exp2(top - fresh)
                e = jnp.exp2(s - fresh)
                total = jnp.sum(e, axis=0, keepdims=True)
                if not first:
                    total = total + totals[:, lo:lo + size] * scale
                tops[:, lo:lo + size] = fresh
                totals[:, lo:lo + size] = total
                return tile, scale, e.astype(jnp.bfloat16)

            def mix(tile, scale, e):
                return tile, scale, jnp.dot(values, e, preferred_element_type=jnp.float32)

            def gather(tile, scale, pv):
                lo, size = tile
                if not first:
                    pv = pv + acc[:, lo:lo + size] * scale
                acc[:, lo:lo + size] = pv

            ready = [score(tile) for tile in tiles[:AHEAD]]
            mixed = []
            for index, tile in enumerate(tiles):
                if index + AHEAD < len(tiles):
                    ready.append(score(tiles[index + AHEAD]))
                mixed.append(mix(*weigh(tile, ready.pop(0))))
                if len(mixed) > BACK:
                    gather(*mixed.pop(0))
            while mixed:
                gather(*mixed.pop(0))

        block(kv_ref, 0, True)
        middle = (behind + 1) // 2

        def between():
            forward(right, across, 0)
            forward(1 - right, home, 0)

        @pl.when((part == 1) & inner & (middle == 0))
        def _():
            between()

        @pl.loop(1, behind + 1)
        def _(away):
            @pl.when((part == 0) & (lax.rem(away, 2) == 1))
            def _():
                kv_copy(away).wait_recv()

            @pl.when((part == 1) & inner & (away == middle))
            def _():
                between()

            block(kv_in.at[away - 1], away, False)

        whole = acc[...] * (1.0 / totals[...])
        context = jnp.concatenate(
            [whole[:, h * chunk:(h + 1) * chunk].T.astype(jnp.bfloat16) for h in range(heads)], axis=1
        )
        ctx[cut, :] = context

        @pl.when((part == 1) & outer)
        def _():
            for index in range(SUBS, 2 * SUBS):
                ctx_copy(index).start()
            for index in range(SUBS):
                term_copy(right, beside, index).start()

        @pl.when(part == 0)
        def _():
            load.wait()

        for dest in range(tp_count):
            sent[dest, cut] = jnp.dot(
                context, wo[:, dest * cols:(dest + 1) * cols], preferred_element_type=jnp.float32
            ).astype(jnp.bfloat16)

        @pl.when((part == 0) & outer)
        def _():
            for index in range(SUBS):
                term_copy(right, across, index).start()
                term_copy(right, farther, index).start()

        @pl.when((part == 0) & inner)
        def _():
            spread(mine, 1, partner).wait_recv()
            for copy in own_spreads():
                copy.start()
            forward(right, far, 0)

    @pl.loop(0, 2)
    def _(part):
        piece(part)

    @pl.when(inner)
    def _():
        for index in range(1, SUBS):
            forward(right, far, index)
            forward(right, across, index)
            forward(1 - right, home, index)
        for copy in passed_spreads():
            copy.wait_recv()
            copy.start()
        other = mine + 1 - 2 * lax.rem(mine, 2)
        for away in [0] + steps:
            spread(lax.rem(other + away, team), 1, partner).wait_recv()

        @pl.loop(SUBS, 2 * SUBS)
        def _(index):
            cut = sub_cut(index)
            ctx_copy(index).wait_recv()
            guest = ctx_in[cut, :]
            for at in range(tp_count - 1):
                dest = at + 1 - right
                sent[dest, cut] = (
                    sent[dest, cut].astype(jnp.float32)
                    + jnp.dot(
                        guest, lent[:, at * cols:(at + 1) * cols], preferred_element_type=jnp.float32
                    )
                ).astype(jnp.bfloat16)
            term_copy(right, far, index).start()
            term_copy(right, across, index).start()

        for index in range(SUBS, 2 * SUBS):
            forward(1 - right, home, index)

    @pl.loop(0, 2 * SUBS)
    def _(index):
        cut = sub_cut(index)
        term_copy(1 - right, turn, index).wait_recv()
        total = sent[turn, cut].astype(jnp.float32) + got[1 - right, turn, cut].astype(jnp.float32)
        both = inner & (index < SUBS)

        @pl.when(both)
        def _():
            term_copy(right, turn, index).wait_recv()
            out_ref[cut, :] = (total + got[right, turn, cut].astype(jnp.float32)).astype(jnp.bfloat16)

        @pl.when(jnp.logical_not(both))
        def _():
            out_ref[cut, :] = total.astype(jnp.bfloat16)

    @pl.loop(0, 2 * SUBS)
    def _(index):
        @pl.when(inner | (index < SUBS))
        def _():
            for dest in range(tp_count):
                @pl.when(dest != turn)
                def _():
                    term_copy(right, dest, index).wait_send()

        @pl.when(outer & (index >= SUBS))
        def _():
            ctx_copy(index).wait_send()

    @pl.when(outer)
    def _():
        lend().wait_send()

    @pl.when(inner)
    def _():
        for copy in own_spreads() + passed_spreads():
            copy.wait_send()

    each_send(lambda copy: copy.wait_send())
    each_relay(lambda copy: copy.wait_send())


def body(
    tokens, norm_gain, q_weight, q_bias, k_weight, k_bias, v_weight, v_bias, o_weight, doc_ids
):
    rows, model = tokens.shape
    seq_count = lax.axis_size("seq")
    tp_count = lax.axis_size("tp")
    width = q_weight.shape[1]
    cols = o_weight.shape[1] // tp_count
    reach = min(seq_count - 1, (seq_count * rows // 2 + 2 * rows - 2) // rows)
    chunk = rows // 2
    team = math.gcd(seq_count, 8)
    subs = rows // chunk * SUBS
    parts = rows // chunk
    near, far = rope_tables(rows, seq_count)
    hbm = pl.BlockSpec(memory_space=pl.ANY)
    vmem = pl.BlockSpec(memory_space=VMEM)
    slots = reach + 1
    spans = -(-width // (2 * HD))
    kdoc = doc_ids.reshape(seq_count, 1, rows)
    return pl.pallas_call(
        functools.partial(attend, seq_count, tp_count, reach, chunk, team),
        out_shape=jax.ShapeDtypeStruct((rows, cols), jnp.bfloat16),
        in_specs=[hbm, vmem, hbm, vmem, hbm, vmem, hbm, vmem, hbm, vmem, hbm, vmem],
        out_specs=vmem,
        scratch_shapes=[
            VMEM((rows, model), jnp.bfloat16),
            VMEM((rows, model), jnp.bfloat16),
            VMEM((model, width), jnp.bfloat16),
            VMEM((model, 2 * HD), jnp.bfloat16),
            VMEM(o_weight.shape, jnp.bfloat16),
            VMEM((2, rows, HD), jnp.float32),
            VMEM((parts, 2 * HD, width // HD * chunk), jnp.bfloat16),
            VMEM((2, rows, HD), jnp.bfloat16),
            VMEM((slots, 2, rows, HD), jnp.bfloat16),
            VMEM((slots, rows, HD), jnp.bfloat16),
            VMEM((HD, width // HD * chunk), jnp.float32),
            VMEM((1, width // HD * chunk), jnp.float32),
            VMEM((1, width // HD * chunk), jnp.float32),
            VMEM((rows, width), jnp.bfloat16),
            VMEM((rows, width), jnp.bfloat16),
            VMEM((width, (tp_count - 1) * cols), jnp.bfloat16),
            VMEM((tp_count, rows, cols), jnp.bfloat16),
            VMEM((2, tp_count, rows, cols), jnp.bfloat16),
            pltpu.SemaphoreType.DMA((8 + spans,)),
            pltpu.SemaphoreType.DMA((slots,)),
            pltpu.SemaphoreType.DMA((slots,)),
            pltpu.SemaphoreType.DMA((slots,)),
            pltpu.SemaphoreType.DMA((tp_count, subs)),
            pltpu.SemaphoreType.DMA((2, tp_count, subs)),
            pltpu.SemaphoreType.DMA((subs,)),
            pltpu.SemaphoreType.DMA((subs,)),
            pltpu.SemaphoreType.DMA((2 * team,)),
            pltpu.SemaphoreType.DMA((team,)),
        ],
        compiler_params=pltpu.CompilerParams(
            collective_id=0, has_side_effects=True, vmem_limit_bytes=56 * 1024 * 1024
        ),
    )(
        tokens, norm_gain, q_weight, q_bias, k_weight, k_bias, v_weight, v_bias, o_weight,
        kdoc, jnp.asarray(near), jnp.asarray(far),
    )


def solution(mesh):
    placed = (
        P("seq", None),
        P(),
        P(None, "tp"),
        P("tp"),
        P(None, "tp"),
        P("tp"),
        P(None, "tp"),
        P("tp"),
        P("tp", None),
        P(),
    )
    return jax.shard_map(
        body, mesh=mesh, in_specs=placed, out_specs=P("seq", "tp"), check_vma=False
    )
```

```python
import functools
import math

import jax
import jax.numpy as jnp
import numpy as np
from jax import lax
from jax.experimental import pallas as pl
from jax.experimental.pallas import tpu as pltpu
from jax.sharding import PartitionSpec as P

HD = 128
MESH = pl.DeviceIdType.MESH
rope_base = 1000000.0
VMEM = pltpu.VMEM
SUBS = 2
AHEAD = 3
BACK = 1


def rope_tables(rows, blocks):
    half = HD // 2
    inv = rope_base ** (-(np.arange(half, dtype=np.float64) * 2.0) / HD)
    inv = np.concatenate([inv, inv])[None, :]
    near = np.arange(rows)[:, None] * inv
    far = np.arange(blocks)[:, None] * rows * inv
    near = np.stack([np.cos(near), np.sin(near)]).astype(np.float32)
    far = np.stack([np.cos(far), np.sin(far)])[:, :, None, :].astype(np.float32)
    return near, far


def attend(
    seq_count, tp_count, reach, chunk, team,
    tokens_hbm, gain_ref, wq_hbm, qb_ref, wk_hbm, kb_ref, wv_hbm, vb_ref, wo_hbm,
    kdoc_ref, near_hbm, far_ref, out_ref,
    tokens, normed, wq, wkv, wo, near, q_ref, kv_ref, kv_in, kext, acc, tops, totals, ctx, ctx_in, lent, sent, got,
    load_sems, kv_send, kv_pass, kv_recv, kv_back, send_sem, recv_sem, ctx_send, ctx_recv, lent_send, lent_recv,
):
    place = lax.axis_index("seq")
    turn = lax.axis_index("tp")
    rows, width = tokens.shape[0], wq.shape[1]
    heads = width // HD
    cols = out_ref.shape[1]
    parts = rows // chunk
    factor = math.log2(math.e) / HD**0.5
    step = 2 * HD
    spans = [(lo, min(step, width - lo)) for lo in range(0, width, step)]
    slab = rows // 4
    token_loads = [
        pltpu.make_async_copy(
            tokens_hbm.at[pl.ds(index * slab, slab)], tokens.at[pl.ds(index * slab, slab)],
            load_sems.at[index],
        )
        for index in range(4)
    ]
    near_load = pltpu.make_async_copy(near_hbm, near, load_sems.at[4])
    kv_loads = [
        pltpu.make_async_copy(wk_hbm, wkv.at[:, pl.ds(0, HD)], load_sems.at[5]),
        pltpu.make_async_copy(wv_hbm, wkv.at[:, pl.ds(HD, HD)], load_sems.at[6]),
    ]
    q_loads = [
        pltpu.make_async_copy(
            wq_hbm.at[:, pl.ds(lo, size)], wq.at[:, pl.ds(lo, size)], load_sems.at[7 + index]
        )
        for index, (lo, size) in enumerate(spans)
    ]
    load = pltpu.make_async_copy(wo_hbm, wo, load_sems.at[7 + len(spans)])
    for copy in token_loads + kv_loads + [near_load]:
        copy.start()

    barrier = pltpu.get_barrier_semaphore()
    span = min(reach + 1, seq_count - 1)
    for away in range(1, span + 1):
        @pl.when(place >= away)
        def _():
            pl.semaphore_signal(barrier, inc=1, device_id={"seq": place - away}, device_id_type=MESH)

        @pl.when(place + away < seq_count)
        def _():
            pl.semaphore_signal(barrier, inc=1, device_id={"seq": place + away}, device_id_type=MESH)

    @pl.when(turn > 0)
    def _():
        pl.semaphore_signal(barrier, inc=1, device_id={"tp": turn - 1}, device_id_type=MESH)

    @pl.when(turn < tp_count - 1)
    def _():
        pl.semaphore_signal(barrier, inc=1, device_id={"tp": turn + 1}, device_id_type=MESH)

    behind = jnp.minimum(place, reach)
    near_count = jnp.minimum(place, span) + jnp.minimum(seq_count - 1 - place, span)
    sides = jnp.where(turn > 0, 1, 0) + jnp.where(turn < tp_count - 1, 1, 0)

    lane = lax.broadcasted_iota(jnp.int32, (rows, HD), 1)
    doc = lax.broadcasted_iota(jnp.int32, (HD, rows), 0)
    for away in range(reach + 1):
        ids = kdoc_ref[jnp.maximum(place - away, 0)]
        kext[away] = jnp.where(doc == ids, 1.0, 0.0).T.astype(jnp.bfloat16)
        if away == 0:
            veto = jnp.where(doc == ids, 0.0, -1e30).astype(jnp.bfloat16)
            for part in range(parts):
                q_ref[part, HD:, :] = jnp.concatenate([veto[:, part * chunk:(part + 1) * chunk]] * heads, axis=1)

    pl.semaphore_wait(barrier, near_count + sides)
    half = tp_count // 2
    right = turn // half
    inner = (turn > 0) & (turn < tp_count - 1)
    outer = jnp.logical_not(inner)
    share = width // team
    mine = lax.rem(place, team)
    base = place - mine
    partner = place + 1 - 2 * lax.rem(place, 2)
    lent_cols = (tp_count - 1) * cols
    steps = list(range(2, team, 2))

    def lend():
        rows_cut = pl.ds(pl.multiple_of(mine * share, 16), share)
        cols_cut = pl.ds(pl.multiple_of((1 - right) * cols, HD), lent_cols)
        return pltpu.make_async_remote_copy(
            src_ref=wo_hbm.at[rows_cut, cols_cut], dst_ref=lent.at[rows_cut],
            send_sem=lent_send.at[0], recv_sem=lent_recv.at[mine],
            device_id={"tp": turn + 1 - 2 * right}, device_id_type=MESH,
        )

    def spread(piece_of, slot, target):
        rows_cut = pl.ds(pl.multiple_of(piece_of * share, 16), share)
        return pltpu.make_async_remote_copy(
            src_ref=lent.at[rows_cut], dst_ref=lent.at[rows_cut],
            send_sem=lent_send.at[slot], recv_sem=lent_recv.at[piece_of],
            device_id={"seq": target}, device_id_type=MESH,
        )

    def own_spreads():
        return [spread(mine, 1, partner)] + [
            spread(mine, 2 + index, base + lax.rem(mine + away, team))
            for index, away in enumerate(steps)
        ]

    def passed_spreads():
        return [
            spread(lax.rem(mine + team - away, team), 2 + len(steps) + index, partner)
            for index, away in enumerate(steps)
        ]

    @pl.when(outer)
    def _():
        lend().start()

    gain = gain_ref[...].reshape(1, gain_ref.shape[0])
    for index in range(4):
        token_loads[index].wait()
        if index == 3:
            for copy in q_loads:
                copy.start()

        @pl.loop(0, slab // 64)
        def _(step):
            cut = pl.ds(pl.multiple_of(index * slab + step * 64, 64), 64)
            wide = tokens[cut, :].astype(jnp.float32)
            mean = jnp.mean(wide * wide, axis=-1, keepdims=True)
            normed[cut, :] = (wide * lax.rsqrt(mean + 1e-06) * gain).astype(jnp.bfloat16)

    near_load.wait()
    far_cos, far_sin = far_ref[0, place], far_ref[1, place]
    cos = near[0] * far_cos - near[1] * far_sin
    sin = near[1] * far_cos + near[0] * far_sin
    near[0] = cos
    near[1] = jnp.where(lane < HD // 2, -sin, sin)

    def rope(t):
        return t * near[0] + pltpu.roll(t, HD // 2, 1) * near[1]

    for copy in kv_loads:
        copy.wait()
    kv = jnp.dot(normed[...], wkv[...], preferred_element_type=jnp.float32)
    kv_ref[0] = rope(kv[:, :HD] + kb_ref[...].reshape(1, HD)).astype(jnp.bfloat16)
    values = kv[:, HD:] + vb_ref[...].reshape(1, HD)
    for lo in range(0, rows, HD):
        kv_ref[1, lo:lo + HD] = values[lo:lo + HD].T.astype(jnp.bfloat16)

    odd = lax.rem(place, 2) == 1

    core = lax.rem(place, 2)
    bent = lax.rem(place // 2, 2) == 1
    bends = reach >= 4

    def kv_copy(away, part):
        return pltpu.make_async_remote_copy(
            src_ref=kv_ref.at[part], dst_ref=kv_in.at[away - 1, part],
            send_sem=kv_send.at[away - 1, part], recv_sem=kv_recv.at[away - 1, part],
            device_id={"seq": lax.rem(place + away, seq_count)}, device_id_type=MESH,
        )

    def relay(away, landing, part):
        return pltpu.make_async_remote_copy(
            src_ref=kv_in.at[away - 1, part], dst_ref=kv_in.at[landing - 1, part],
            send_sem=kv_pass.at[away - 1, part], recv_sem=kv_recv.at[landing - 1, part],
            device_id={"seq": partner}, device_id_type=MESH,
        )

    def back(part):
        return pltpu.make_async_remote_copy(
            src_ref=kv_in.at[3, part], dst_ref=kv_in.at[1, part],
            send_sem=kv_back.at[part], recv_sem=kv_recv.at[1, part],
            device_id={"seq": lax.rem(place + seq_count - 2, seq_count)}, device_id_type=MESH,
        )

    evens = [away for away in range(2, reach + 2, 2) if away < seq_count]
    backs = bent & (place >= 4) & bends

    def wanted(away):
        return odd if away > reach else (place >= 0)

    def each_send(act):
        for part in (0, 1):
            for away in evens:
                direct = jnp.logical_not(bent & (place + 4 < seq_count) & bends & (away == 2))

                @pl.when((place + away < seq_count) & wanted(away) & direct)
                def _():
                    act(kv_copy(away, part))

            @pl.when(jnp.logical_not(odd))
            def _():
                act(kv_copy(1, part))

    def each_relay(act):
        for part in (0, 1):
            for away in evens:
                if away + 1 <= reach:
                    @pl.when((place >= away) & jnp.logical_not(odd))
                    def _():
                        act(relay(away, away + 1, part))

                @pl.when((place >= away) & odd)
                def _():
                    act(relay(away, away - 1, part))

            if bends:
                @pl.when(backs)
                def _():
                    act(back(part))

    def take(group):
        for part in (0, 1):
            @pl.when(jnp.logical_not(backs & (group == 4)))
            def _():
                kv_copy(group, part).wait_recv()

            @pl.when(odd | (group + 1 <= reach))
            def _():
                relay(group, group + 1 - 2 * core, part).start()

    def obtain(away):
        even = lax.rem(away, 2) == 0

        @pl.when(even & (jnp.logical_not(odd) | (away == behind)))
        def _():
            take(away)

        @pl.when(jnp.logical_not(even) & odd & (away > 2))
        def _():
            take(away - 1)

        if evens and evens[-1] > reach:
            @pl.when((away == 1) & odd & (place >= evens[-1]))
            def _():
                take(evens[-1])

        @pl.when(jnp.logical_not(even))
        def _():
            for part in (0, 1):
                kv_copy(away, part).wait_recv()

    def bounce(part):
        if bends:
            @pl.when(backs)
            def _():
                kv_copy(4, part).wait_recv()
                back(part).start()

    each_send(lambda copy: copy.start())

    for index in range(0, len(spans), 2):
        for copy in q_loads[index:index + 2]:
            copy.wait()
        if index == 0:
            load.start()
        lo = spans[index][0]
        size = sum(extent for _, extent in spans[index:index + 2])
        out = jnp.dot(
            normed[...], wq[:, lo:lo + size], preferred_element_type=jnp.float32
        ) + qb_ref[lo:lo + size].reshape(1, size)
        for head in range(0, size, HD):
            turned = rope(out[:, head:head + HD]) * factor
            at = (lo + head) // HD * chunk
            for part in range(parts):
                q_ref[part, :HD, at:at + chunk] = turned[part * chunk:(part + 1) * chunk].T.astype(jnp.bfloat16)

    def offer():
        spread(mine, 1, partner).wait_recv()
        for copy in own_spreads():
            copy.start()

    sub = chunk // SUBS

    def sub_cut(index):
        return pl.ds(pl.multiple_of(index * sub, sub), sub)

    def term_copy(side, dest, index):
        return pltpu.make_async_remote_copy(
            src_ref=sent.at[dest, sub_cut(index)], dst_ref=got.at[side, dest, sub_cut(index)],
            send_sem=send_sem.at[dest, index], recv_sem=recv_sem.at[side, dest, index],
            device_id={"tp": turn + 1 - 2 * side}, device_id_type=MESH,
        )

    def ctx_copy(index):
        return pltpu.make_async_remote_copy(
            src_ref=ctx.at[sub_cut(index)], dst_ref=ctx_in.at[sub_cut(index)],
            send_sem=ctx_send.at[index], recv_sem=ctx_recv.at[index],
            device_id={"tp": turn + 1 - 2 * right}, device_id_type=MESH,
        )

    last = tp_count - 1
    far = (1 - right) * last
    home = right * last
    across = last - turn
    farther = (1 - right) * (last - 1) + right
    beside = (1 - right) + right * (last - 1)

    def forward(side, dest, index):
        cut = sub_cut(index)
        term_copy(side, dest, index).wait_recv()
        sent[dest, cut] = (
            sent[dest, cut].astype(jnp.float32) + got[side, dest, cut].astype(jnp.float32)
        ).astype(jnp.bfloat16)
        term_copy(side, dest, index).start()

    wide = step // chunk * chunk
    tiles = [(lo, min(wide, heads * chunk - lo)) for lo in range(0, heads * chunk, wide)]

    def piece(part):
        cut = pl.ds(pl.multiple_of(part * chunk, chunk), chunk)
        def block(held, away, first):
            keys = jnp.concatenate([held[0], kext[away]], axis=1)
            values = jnp.concatenate([held[1, lo:lo + HD] for lo in range(0, rows, HD)], axis=1)
            if first:
                key = lax.broadcasted_iota(jnp.int32, (rows, chunk), 0)
                row = part * chunk + lax.broadcasted_iota(jnp.int32, (rows, chunk), 1)
                later = jnp.where(key <= row, 0.0, -1e30)
            def score(tile):
                lo, size = tile
                s = jnp.dot(keys, q_ref[part, :, lo:lo + size], preferred_element_type=jnp.float32)
                if first:
                    s = s + jnp.concatenate([later] * (size // chunk), axis=1)
                return s

            def weigh(tile, s):
                lo, size = tile
                fresh = jnp.max(s, axis=0, keepdims=True)
                scale = None
                if not first:
                    top = tops[:, lo:lo + size]
                    fresh = jnp.maximum(top, fresh)
                    scale = jnp.exp2(top - fresh)
                e = jnp.exp2(s - fresh)
                total = jnp.sum(e, axis=0, keepdims=True)
                if not first:
                    total = total + totals[:, lo:lo + size] * scale
                tops[:, lo:lo + size] = fresh
                totals[:, lo:lo + size] = total
                return tile, scale, e.astype(jnp.bfloat16)

            def mix(tile, scale, e):
                return tile, scale, jnp.dot(values, e, preferred_element_type=jnp.float32)

            def gather(tile, scale, pv):
                lo, size = tile
                if not first:
                    pv = pv + acc[:, lo:lo + size] * scale
                acc[:, lo:lo + size] = pv

            ready = [score(tile) for tile in tiles[:AHEAD]]
            mixed = []
            for index, tile in enumerate(tiles):
                if index + AHEAD < len(tiles):
                    ready.append(score(tiles[index + AHEAD]))
                mixed.append(mix(*weigh(tile, ready.pop(0))))
                if len(mixed) > BACK:
                    gather(*mixed.pop(0))
            while mixed:
                gather(*mixed.pop(0))

        @pl.when(part == 0)
        def _():
            bounce(0)

        block(kv_ref, 0, True)
        middle = (behind + 1) // 2

        def between():
            forward(right, far, 1)
            forward(1 - right, home, 0)

        @pl.when(part == 0)
        def _():
            bounce(1)

        @pl.when((part == 1) & inner & (middle == 0))
        def _():
            between()

        tail = (1 - core) * (behind // reach) * (reach % 2) if reach else 0

        @pl.loop(1, behind + 1)
        def _(turned):
            away = lax.rem(2 * behind - turned - tail, behind) + 1

            @pl.when(part == 0)
            def _():
                obtain(away)

            @pl.when((part == 1) & inner & (turned == middle))
            def _():
                between()

            block(kv_in.at[away - 1], away, False)

        @pl.when((part == 0) & inner & (behind > 1))
        def _():
            offer()

        whole = acc[...] * (1.0 / totals[...])
        context = jnp.concatenate(
            [whole[:, h * chunk:(h + 1) * chunk].T.astype(jnp.bfloat16) for h in range(heads)], axis=1
        )
        ctx[cut, :] = context

        @pl.when((part == 1) & outer)
        def _():
            for index in range(SUBS, 2 * SUBS):
                ctx_copy(index).start()
            for index in range(SUBS):
                term_copy(right, beside, index).start()

        @pl.when(part == 0)
        def _():
            load.wait()

        for dest in range(tp_count):
            sent[dest, cut] = jnp.dot(
                context, wo[:, dest * cols:(dest + 1) * cols], preferred_element_type=jnp.float32
            ).astype(jnp.bfloat16)

        @pl.when((part == 0) & outer)
        def _():
            for dest in (across, farther):
                for index in range(SUBS):
                    term_copy(right, dest, index).start()

        @pl.when((part == 0) & inner & (behind < 2))
        def _():
            offer()

        @pl.when((part == 0) & inner)
        def _():
            forward(right, far, 0)

    @pl.loop(0, 2)
    def _(part):
        piece(part)

    @pl.when(inner)
    def _():
        for index in range(2, SUBS):
            forward(right, far, index)
        for index in range(SUBS):
            forward(right, across, index)
        for index in range(1, SUBS):
            forward(1 - right, home, index)
        for copy in passed_spreads():
            copy.wait_recv()
            copy.start()
        other = mine + 1 - 2 * lax.rem(mine, 2)
        for away in [0] + steps:
            spread(lax.rem(other + away, team), 1, partner).wait_recv()

        @pl.loop(SUBS, 2 * SUBS)
        def _(index):
            cut = sub_cut(index)
            ctx_copy(index).wait_recv()
            guest = ctx_in[cut, :]
            for at in range(tp_count - 1):
                dest = at + 1 - right
                sent[dest, cut] = (
                    sent[dest, cut].astype(jnp.float32)
                    + jnp.dot(
                        guest, lent[:, at * cols:(at + 1) * cols], preferred_element_type=jnp.float32
                    )
                ).astype(jnp.bfloat16)
            term_copy(right, far, index).start()

        for index in range(SUBS, 2 * SUBS):
            term_copy(right, across, index).start()
        for index in range(SUBS, 2 * SUBS):
            forward(1 - right, home, index)

    @pl.loop(0, 2 * SUBS)
    def _(index):
        cut = sub_cut(index)
        term_copy(1 - right, turn, index).wait_recv()
        total = sent[turn, cut].astype(jnp.float32) + got[1 - right, turn, cut].astype(jnp.float32)
        both = inner & (index < SUBS)

        @pl.when(both)
        def _():
            term_copy(right, turn, index).wait_recv()
            out_ref[cut, :] = (total + got[right, turn, cut].astype(jnp.float32)).astype(jnp.bfloat16)

        @pl.when(jnp.logical_not(both))
        def _():
            out_ref[cut, :] = total.astype(jnp.bfloat16)

    @pl.loop(0, 2 * SUBS)
    def _(index):
        @pl.when(inner | (index < SUBS))
        def _():
            for dest in range(tp_count):
                @pl.when(dest != turn)
                def _():
                    term_copy(right, dest, index).wait_send()

        @pl.when(outer & (index >= SUBS))
        def _():
            ctx_copy(index).wait_send()

    @pl.when(outer)
    def _():
        lend().wait_send()

    @pl.when(inner)
    def _():
        for copy in own_spreads() + passed_spreads():
            copy.wait_send()

    each_send(lambda copy: copy.wait_send())
    each_relay(lambda copy: copy.wait_send())


def body(
    tokens, norm_gain, q_weight, q_bias, k_weight, k_bias, v_weight, v_bias, o_weight, doc_ids
):
    rows, model = tokens.shape
    seq_count = lax.axis_size("seq")
    tp_count = lax.axis_size("tp")
    width = q_weight.shape[1]
    cols = o_weight.shape[1] // tp_count
    reach = min(seq_count - 1, (seq_count * rows // 2 + 2 * rows - 2) // rows)
    chunk = rows // 2
    team = math.gcd(seq_count, 8)
    subs = rows // chunk * SUBS
    parts = rows // chunk
    near, far = rope_tables(rows, seq_count)
    hbm = pl.BlockSpec(memory_space=pl.ANY)
    vmem = pl.BlockSpec(memory_space=VMEM)
    slots = reach + 1
    spans = -(-width // (2 * HD))
    kdoc = doc_ids.reshape(seq_count, 1, rows)
    return pl.pallas_call(
        functools.partial(attend, seq_count, tp_count, reach, chunk, team),
        out_shape=jax.ShapeDtypeStruct((rows, cols), jnp.bfloat16),
        in_specs=[hbm, vmem, hbm, vmem, hbm, vmem, hbm, vmem, hbm, vmem, hbm, vmem],
        out_specs=vmem,
        scratch_shapes=[
            VMEM((rows, model), jnp.bfloat16),
            VMEM((rows, model), jnp.bfloat16),
            VMEM((model, width), jnp.bfloat16),
            VMEM((model, 2 * HD), jnp.bfloat16),
            VMEM(o_weight.shape, jnp.bfloat16),
            VMEM((2, rows, HD), jnp.float32),
            VMEM((parts, 2 * HD, width // HD * chunk), jnp.bfloat16),
            VMEM((2, rows, HD), jnp.bfloat16),
            VMEM((slots, 2, rows, HD), jnp.bfloat16),
            VMEM((slots, rows, HD), jnp.bfloat16),
            VMEM((HD, width // HD * chunk), jnp.float32),
            VMEM((1, width // HD * chunk), jnp.float32),
            VMEM((1, width // HD * chunk), jnp.float32),
            VMEM((rows, width), jnp.bfloat16),
            VMEM((rows, width), jnp.bfloat16),
            VMEM((width, (tp_count - 1) * cols), jnp.bfloat16),
            VMEM((tp_count, rows, cols), jnp.bfloat16),
            VMEM((2, tp_count, rows, cols), jnp.bfloat16),
            pltpu.SemaphoreType.DMA((8 + spans,)),
            pltpu.SemaphoreType.DMA((slots, 2)),
            pltpu.SemaphoreType.DMA((slots, 2)),
            pltpu.SemaphoreType.DMA((slots, 2)),
            pltpu.SemaphoreType.DMA((2,)),
            pltpu.SemaphoreType.DMA((tp_count, subs)),
            pltpu.SemaphoreType.DMA((2, tp_count, subs)),
            pltpu.SemaphoreType.DMA((subs,)),
            pltpu.SemaphoreType.DMA((subs,)),
            pltpu.SemaphoreType.DMA((2 * team,)),
            pltpu.SemaphoreType.DMA((team,)),
        ],
        compiler_params=pltpu.CompilerParams(
            collective_id=0, has_side_effects=True, vmem_limit_bytes=56 * 1024 * 1024
        ),
    )(
        tokens, norm_gain, q_weight, q_bias, k_weight, k_bias, v_weight, v_bias, o_weight,
        kdoc, jnp.asarray(near), jnp.asarray(far),
    )


def solution(mesh):
    placed = (
        P("seq", None),
        P(),
        P(None, "tp"),
        P("tp"),
        P(None, "tp"),
        P("tp"),
        P(None, "tp"),
        P("tp"),
        P("tp", None),
        P(),
    )
    return jax.shard_map(
        body, mesh=mesh, in_specs=placed, out_specs=P("seq", "tp"), check_vma=False
    )
```

```python
import functools
import math

import jax
import jax.numpy as jnp
import numpy as np
from jax import lax
from jax.experimental import pallas as pl
from jax.experimental.pallas import tpu as pltpu
from jax.sharding import PartitionSpec as P

HD = 128
MESH = pl.DeviceIdType.MESH
rope_base = 1000000.0
VMEM = pltpu.VMEM
SUBS = 4
TERMS = 5
AHEAD = 3
BACK = 1


def rope_tables(rows, blocks):
    half = HD // 2
    inv = rope_base ** (-(np.arange(half, dtype=np.float64) * 2.0) / HD)
    inv = np.concatenate([inv, inv])[None, :]
    near = np.arange(rows)[:, None] * inv
    far = np.arange(blocks)[:, None] * rows * inv
    near = np.stack([np.cos(near), np.sin(near)]).astype(np.float32)
    far = np.stack([np.cos(far), np.sin(far)])[:, :, None, :].astype(np.float32)
    return near, far


def attend(
    seq_count, tp_count, reach, chunk, team,
    tokens_hbm, gain_hbm, wq_hbm, qb_hbm, wk_hbm, kb_hbm, wv_hbm, vb_hbm, wo_hbm,
    kdoc_hbm, near_hbm, far_hbm, out_ref,
    gain_ref, qb_ref, kb_ref, vb_ref, kdoc_ref, far_ref, tokens, normed, wq, wkv, wo, near, q_ref, kv_ref, kv_in, kext, acc, tops, totals, ctx, ctx_in, lent, sent, got,
    load_sems, kv_send, kv_pass, kv_recv, kv_back, send_sem, recv_sem, ctx_send, ctx_recv, lent_send, lent_recv,
):
    place = lax.axis_index("seq")
    turn = lax.axis_index("tp")
    rows, width = tokens.shape[0], wq.shape[1]
    heads = width // HD
    cols = out_ref.shape[1]
    parts = rows // chunk
    factor = math.log2(math.e) / HD**0.5
    step = 2 * HD
    spans = [(lo, min(step, width - lo)) for lo in range(0, width, step)]
    slab = rows // 4
    token_loads = [
        pltpu.make_async_copy(
            tokens_hbm.at[pl.ds(index * slab, slab)], tokens.at[pl.ds(index * slab, slab)],
            load_sems.at[index],
        )
        for index in range(4)
    ]
    near_load = pltpu.make_async_copy(near_hbm, near, load_sems.at[4])
    kv_loads = [
        pltpu.make_async_copy(wk_hbm, wkv.at[:, pl.ds(0, HD)], load_sems.at[5]),
        pltpu.make_async_copy(wv_hbm, wkv.at[:, pl.ds(HD, HD)], load_sems.at[6]),
    ]
    q_loads = [
        pltpu.make_async_copy(
            wq_hbm.at[:, pl.ds(lo, size)], wq.at[:, pl.ds(lo, size)], load_sems.at[7 + index]
        )
        for index, (lo, size) in enumerate(spans)
    ]
    load = pltpu.make_async_copy(wo_hbm, wo, load_sems.at[7 + len(spans)])
    small = [
        pltpu.make_async_copy(source, target, load_sems.at[8 + len(spans) + index])
        for index, (source, target) in enumerate([
            (kdoc_hbm, kdoc_ref), (gain_hbm, gain_ref), (far_hbm, far_ref),
            (kb_hbm, kb_ref), (vb_hbm, vb_ref), (qb_hbm, qb_ref),
        ])
    ]
    for copy in small + token_loads + kv_loads + [near_load]:
        copy.start()

    barrier = pltpu.get_barrier_semaphore()
    span = min(reach + 1, seq_count - 1)
    for away in range(1, span + 1):
        @pl.when(place >= away)
        def _():
            pl.semaphore_signal(barrier, inc=1, device_id={"seq": place - away}, device_id_type=MESH)

        @pl.when(place + away < seq_count)
        def _():
            pl.semaphore_signal(barrier, inc=1, device_id={"seq": place + away}, device_id_type=MESH)

    @pl.when(turn > 0)
    def _():
        pl.semaphore_signal(barrier, inc=1, device_id={"tp": turn - 1}, device_id_type=MESH)

    @pl.when(turn < tp_count - 1)
    def _():
        pl.semaphore_signal(barrier, inc=1, device_id={"tp": turn + 1}, device_id_type=MESH)

    behind = jnp.minimum(place, reach)
    near_count = jnp.minimum(place, span) + jnp.minimum(seq_count - 1 - place, span)
    sides = jnp.where(turn > 0, 1, 0) + jnp.where(turn < tp_count - 1, 1, 0)

    small[0].wait()
    lane = lax.broadcasted_iota(jnp.int32, (rows, HD), 1)
    doc = lax.broadcasted_iota(jnp.int32, (HD, rows), 0)
    for away in range(reach + 1):
        ids = kdoc_ref[jnp.maximum(place - away, 0)]
        kext[away] = jnp.where(doc == ids, 1.0, 0.0).T.astype(jnp.bfloat16)
        if away == 0:
            veto = jnp.where(doc == ids, 0.0, -1e30).astype(jnp.bfloat16)
            for part in range(parts):
                q_ref[part, HD:, :] = jnp.concatenate([veto[:, part * chunk:(part + 1) * chunk]] * heads, axis=1)

    pl.semaphore_wait(barrier, near_count + sides)
    half = tp_count // 2
    right = turn // half
    inner = (turn > 0) & (turn < tp_count - 1)
    outer = jnp.logical_not(inner)
    share = width // team
    mine = lax.rem(place, team)
    base = place - mine
    partner = place + 1 - 2 * lax.rem(place, 2)
    lent_cols = (tp_count - 1) * cols
    steps = list(range(2, team, 2))

    def lend():
        rows_cut = pl.ds(pl.multiple_of(mine * share, 16), share)
        cols_cut = pl.ds(pl.multiple_of((1 - right) * cols, HD), lent_cols)
        return pltpu.make_async_remote_copy(
            src_ref=wo_hbm.at[rows_cut, cols_cut], dst_ref=lent.at[rows_cut],
            send_sem=lent_send.at[0], recv_sem=lent_recv.at[mine],
            device_id={"tp": turn + 1 - 2 * right}, device_id_type=MESH,
        )

    def spread(piece_of, slot, target):
        rows_cut = pl.ds(pl.multiple_of(piece_of * share, 16), share)
        return pltpu.make_async_remote_copy(
            src_ref=lent.at[rows_cut], dst_ref=lent.at[rows_cut],
            send_sem=lent_send.at[slot], recv_sem=lent_recv.at[piece_of],
            device_id={"seq": target}, device_id_type=MESH,
        )

    def mirror(index, bits):
        moved = index
        bit = 1
        while bit < team:
            if bits // bit % 2:
                moved = moved + bit - 2 * bit * lax.rem(index // bit, 2)
            bit *= 2
        return moved

    straight = [bits for bits in steps if bits & (bits - 1) == 0]

    def own_spreads():
        return [spread(mine, 1, partner)] + [
            spread(mine, 2 + index, base + mirror(mine, bits)) for index, bits in enumerate(straight)
        ]

    def passed_spread(index):
        return spread(mirror(mine, steps[index]), 2 + len(steps) + index, partner)

    def cross():
        a, b = mirror(mine, straight[0]), mirror(mine, straight[-1])
        side = lax.rem(mine, 2)
        return spread((1 - side) * a + side * b, 1 + len(steps), base + (1 - side) * b + side * a)

    def hand_over(wanted_steps):
        for index, bits in enumerate(steps):
            if bits in wanted_steps:
                copy = passed_spread(index)
                copy.wait_recv()
                copy.start()

    bent_steps = [bits for bits in steps if bits not in straight]

    def pass_straight():
        hand_over(straight)
        if bent_steps:
            cross().start()

    @pl.when(outer)
    def _():
        lend().start()

    for copy in small[1:]:
        copy.wait()
    gain = gain_ref[...].reshape(1, gain_ref.shape[0])
    for index in range(4):
        token_loads[index].wait()
        if index == 3:
            for copy in q_loads:
                copy.start()

        @pl.loop(0, slab // 64)
        def _(step):
            cut = pl.ds(pl.multiple_of(index * slab + step * 64, 64), 64)
            wide = tokens[cut, :].astype(jnp.float32)
            mean = jnp.mean(wide * wide, axis=-1, keepdims=True)
            normed[cut, :] = (wide * lax.rsqrt(mean + 1e-06) * gain).astype(jnp.bfloat16)

    near_load.wait()
    far_cos, far_sin = far_ref[0, place], far_ref[1, place]
    cos = near[0] * far_cos - near[1] * far_sin
    sin = near[1] * far_cos + near[0] * far_sin
    near[0] = cos
    near[1] = jnp.where(lane < HD // 2, -sin, sin)

    def rope(t):
        return t * near[0] + pltpu.roll(t, HD // 2, 1) * near[1]

    for copy in kv_loads:
        copy.wait()
    kv = jnp.dot(normed[...], wkv[...], preferred_element_type=jnp.float32)
    kv_ref[0] = rope(kv[:, :HD] + kb_ref[...].reshape(1, HD)).astype(jnp.bfloat16)
    values = kv[:, HD:] + vb_ref[...].reshape(1, HD)
    for lo in range(0, rows, HD):
        kv_ref[1, lo:lo + HD] = values[lo:lo + HD].T.astype(jnp.bfloat16)

    odd = lax.rem(place, 2) == 1

    core = lax.rem(place, 2)
    bent = lax.rem(place // 2, 2) == 1
    bends = reach >= 4

    def kv_copy(away, part):
        return pltpu.make_async_remote_copy(
            src_ref=kv_ref.at[part], dst_ref=kv_in.at[away - 1, part],
            send_sem=kv_send.at[away - 1, part], recv_sem=kv_recv.at[away - 1, part],
            device_id={"seq": lax.rem(place + away, seq_count)}, device_id_type=MESH,
        )

    def relay(away, landing, part):
        return pltpu.make_async_remote_copy(
            src_ref=kv_in.at[away - 1, part], dst_ref=kv_in.at[landing - 1, part],
            send_sem=kv_pass.at[away - 1, part], recv_sem=kv_recv.at[landing - 1, part],
            device_id={"seq": partner}, device_id_type=MESH,
        )

    def back(part):
        return pltpu.make_async_remote_copy(
            src_ref=kv_in.at[3, part], dst_ref=kv_in.at[1, part],
            send_sem=kv_back.at[part], recv_sem=kv_recv.at[1, part],
            device_id={"seq": lax.rem(place + seq_count - 2, seq_count)}, device_id_type=MESH,
        )

    evens = [away for away in range(2, reach + 2, 2) if away < seq_count]
    backs = bent & (place >= 4) & bends

    def wanted(away):
        return odd if away > reach else (place >= 0)

    def each_send(act):
        for part in (0, 1):
            for away in evens:
                direct = jnp.logical_not(bent & (place + 4 < seq_count) & bends & (away == 2))

                @pl.when((place + away < seq_count) & wanted(away) & direct)
                def _():
                    act(kv_copy(away, part))

            @pl.when(jnp.logical_not(odd))
            def _():
                act(kv_copy(1, part))

    def each_relay(act):
        for part in (0, 1):
            for away in evens:
                if away + 1 <= reach:
                    @pl.when((place >= away) & jnp.logical_not(odd))
                    def _():
                        act(relay(away, away + 1, part))

                @pl.when((place >= away) & odd)
                def _():
                    act(relay(away, away - 1, part))

            if bends:
                @pl.when(backs)
                def _():
                    act(back(part))

    def take(group):
        for part in (0, 1):
            @pl.when(jnp.logical_not(backs & (group == 4)))
            def _():
                kv_copy(group, part).wait_recv()

            @pl.when(odd | (group + 1 <= reach))
            def _():
                relay(group, group + 1 - 2 * core, part).start()

    def obtain(away):
        even = lax.rem(away, 2) == 0

        @pl.when(even & (jnp.logical_not(odd) | (away == behind)))
        def _():
            take(away)

        @pl.when(jnp.logical_not(even) & odd & (away > 2))
        def _():
            take(away - 1)

        if evens and evens[-1] > reach:
            @pl.when((away == 2) & odd & (place >= evens[-1]))
            def _():
                take(evens[-1])

        @pl.when(jnp.logical_not(even))
        def _():
            for part in (0, 1):
                kv_copy(away, part).wait_recv()

    def bounce(part):
        if bends:
            @pl.when(backs)
            def _():
                kv_copy(4, part).wait_recv()
                back(part).start()

    each_send(lambda copy: copy.start())

    for index in range(0, len(spans), 2):
        for copy in q_loads[index:index + 2]:
            copy.wait()
        if index == 0:
            load.start()
        lo = spans[index][0]
        size = sum(extent for _, extent in spans[index:index + 2])
        out = jnp.dot(
            normed[...], wq[:, lo:lo + size], preferred_element_type=jnp.float32
        ) + qb_ref[lo:lo + size].reshape(1, size)
        for head in range(0, size, HD):
            turned = rope(out[:, head:head + HD]) * factor
            at = (lo + head) // HD * chunk
            for part in range(parts):
                q_ref[part, :HD, at:at + chunk] = turned[part * chunk:(part + 1) * chunk].T.astype(jnp.bfloat16)

    def offer():
        spread(mine, 1, partner).wait_recv()
        for copy in own_spreads():
            copy.start()

    sub = chunk // SUBS

    def sub_cut(index):
        return pl.ds(pl.multiple_of(index * sub, sub), sub)

    def term_copy(side, dest, index):
        return pltpu.make_async_remote_copy(
            src_ref=sent.at[dest, sub_cut(index)], dst_ref=got.at[side, dest, sub_cut(index)],
            send_sem=send_sem.at[dest, index], recv_sem=recv_sem.at[side, dest, index],
            device_id={"tp": turn + 1 - 2 * side}, device_id_type=MESH,
        )

    def ctx_copy(index):
        return pltpu.make_async_remote_copy(
            src_ref=ctx.at[sub_cut(index)], dst_ref=ctx_in.at[sub_cut(index)],
            send_sem=ctx_send.at[index], recv_sem=ctx_recv.at[index],
            device_id={"tp": turn + 1 - 2 * right}, device_id_type=MESH,
        )

    last = tp_count - 1
    far = (1 - right) * last
    home = right * last
    farther = (1 - right) * (last - 1) + right
    other = turn + 1 - 2 * lax.rem(turn, 2)

    def forward(side, dest, index):
        cut = sub_cut(index)
        term_copy(side, dest, index).wait_recv()
        sent[dest, cut] = (
            sent[dest, cut].astype(jnp.float32) + got[side, dest, cut].astype(jnp.float32)
        ).astype(jnp.bfloat16)
        term_copy(side, dest, index).start()

    def event(index):
        @pl.when(index < 2 * SUBS)
        def _():
            forward(right, far + index // SUBS * (farther - far), lax.rem(index, SUBS))

        @pl.when((index > 1) & (index < SUBS + 2))
        def _():
            forward(1 - right, home, index - 2)

    wide = step // chunk * chunk
    tiles = [(lo, min(wide, heads * chunk - lo)) for lo in range(0, heads * chunk, wide)]

    def piece(part):
        cut = pl.ds(pl.multiple_of(part * chunk, chunk), chunk)
        def block(held, away, first):
            keys = jnp.concatenate([held[0], kext[away]], axis=1)
            values = jnp.concatenate([held[1, lo:lo + HD] for lo in range(0, rows, HD)], axis=1)
            if first:
                key = lax.broadcasted_iota(jnp.int32, (rows, chunk), 0)
                row = part * chunk + lax.broadcasted_iota(jnp.int32, (rows, chunk), 1)
                later = jnp.where(key <= row, 0.0, -1e30)
            def score(tile):
                lo, size = tile
                s = jnp.dot(keys, q_ref[part, :, lo:lo + size], preferred_element_type=jnp.float32)
                if first:
                    s = s + jnp.concatenate([later] * (size // chunk), axis=1)
                return s

            def weigh(tile, s):
                lo, size = tile
                fresh = jnp.max(s, axis=0, keepdims=True)
                scale = None
                if not first:
                    top = tops[:, lo:lo + size]
                    fresh = jnp.maximum(top, fresh)
                    scale = jnp.exp2(top - fresh)
                e = jnp.exp2(s - fresh)
                total = jnp.sum(e, axis=0, keepdims=True)
                if not first:
                    total = total + totals[:, lo:lo + size] * scale
                tops[:, lo:lo + size] = fresh
                totals[:, lo:lo + size] = total
                return tile, scale, e.astype(jnp.bfloat16)

            def mix(tile, scale, e):
                return tile, scale, jnp.dot(values, e, preferred_element_type=jnp.float32)

            def gather(tile, scale, pv):
                lo, size = tile
                if not first:
                    pv = pv + acc[:, lo:lo + size] * scale
                acc[:, lo:lo + size] = pv

            ready = [score(tile) for tile in tiles[:AHEAD]]
            mixed = []
            for index, tile in enumerate(tiles):
                if index + AHEAD < len(tiles):
                    ready.append(score(tiles[index + AHEAD]))
                mixed.append(mix(*weigh(tile, ready.pop(0))))
                if len(mixed) > BACK:
                    gather(*mixed.pop(0))
            while mixed:
                gather(*mixed.pop(0))

        @pl.when(part == 0)
        def _():
            bounce(0)

        block(kv_ref, 0, True)
        @pl.when(part == 0)
        def _():
            bounce(1)

        tail = (1 - core) * (behind // reach) * (reach % 2) if reach else 0

        @pl.loop(1, behind + 1)
        def _(turned):
            away = lax.rem(2 * behind - turned - tail + core, behind) + 1

            @pl.when(part == 0)
            def _():
                obtain(away)

            @pl.when((part == 0) & inner & (behind > 1) & (turned == behind))
            def _():
                offer()

            @pl.when((part == 1) & inner)
            def _():
                event(turned - 1)

            @pl.when((part == 1) & inner & (turned == behind - 1) & (behind > 4))
            def _():
                pass_straight()

            block(kv_in.at[away - 1], away, False)

        whole = acc[...] * (1.0 / totals[...])
        context = jnp.concatenate(
            [whole[:, h * chunk:(h + 1) * chunk].T.astype(jnp.bfloat16) for h in range(heads)], axis=1
        )
        ctx[cut, :] = context

        @pl.when((part == 1) & inner)
        def _():
            event(behind)

            @pl.when((behind > 1) & (behind < 5))
            def _():
                pass_straight()

        @pl.when(part == 0)
        def _():
            load.wait()

        def term(dest):
            sent[dest, cut] = jnp.dot(
                context, wo[:, pl.ds(pl.multiple_of(dest * cols, HD), cols)],
                preferred_element_type=jnp.float32,
            ).astype(jnp.bfloat16)

        def launch(dest):
            @pl.when((part == 0) & outer)
            def _():
                for index in range(SUBS):
                    term_copy(right, dest, index).start()

            @pl.when((part == 1) & outer)
            def _():
                for index in range(SUBS, TERMS):
                    term_copy(right, dest, index).start()

        term(far)
        launch(far)
        term(farther)
        launch(farther)

        @pl.when((part == 1) & outer)
        def _():
            for index in range(TERMS, 2 * SUBS):
                ctx_copy(index).start()
            for index in range(SUBS):
                term_copy(right, other, index).start()

        term(other)
        term(turn)

        @pl.when((part == 1) & outer)
        def _():
            for index in range(SUBS, TERMS):
                term_copy(right, other, index).start()

        @pl.when((part == 0) & inner & (behind < 2))
        def _():
            offer()

    @pl.loop(0, 2)
    def _(part):
        piece(part)

    @pl.when(inner)
    def _():
        split = jnp.where(behind > 1, behind + 1, 2 * SUBS - 1)
        early = (behind > 4) & (behind < 2 * SUBS - 2)

        @pl.loop(behind + 1, split)
        def _(index):
            event(index)

        @pl.when(behind < 2)
        def _():
            pass_straight()

        @pl.loop(split, 2 * SUBS)
        def _(index):
            event(index)

            @pl.when((index == 2 * SUBS - 2) & early)
            def _():
                hand_over(bent_steps)

        for index in range(SUBS, TERMS):
            forward(right, far, index)
            forward(right, farther, index)

        @pl.when(jnp.logical_not(early))
        def _():
            hand_over(bent_steps)

        twin = mine + 1 - 2 * lax.rem(mine, 2)
        for bits in [0] + steps:
            spread(mirror(twin, bits), 1, partner).wait_recv()

        @pl.loop(TERMS, 2 * SUBS)
        def _(index):
            cut = sub_cut(index)
            ctx_copy(index).wait_recv()
            guest = ctx_in[cut, :]
            for at in range(tp_count - 1):
                dest = at + 1 - right
                sent[dest, cut] = (
                    sent[dest, cut].astype(jnp.float32)
                    + jnp.dot(
                        guest, lent[:, at * cols:(at + 1) * cols], preferred_element_type=jnp.float32
                    )
                ).astype(jnp.bfloat16)
            term_copy(right, far, index).start()

        for index in range(TERMS, 2 * SUBS):
            term_copy(right, farther, index).start()
        for index in range(SUBS, 2 * SUBS):
            forward(1 - right, home, index)

    @pl.loop(0, 2 * SUBS)
    def _(index):
        cut = sub_cut(index)
        term_copy(1 - right, turn, index).wait_recv()
        total = sent[turn, cut].astype(jnp.float32) + got[1 - right, turn, cut].astype(jnp.float32)
        both = inner & (index < TERMS)

        @pl.when(both)
        def _():
            term_copy(right, turn, index).wait_recv()
            out_ref[cut, :] = (total + got[right, turn, cut].astype(jnp.float32)).astype(jnp.bfloat16)

        @pl.when(jnp.logical_not(both))
        def _():
            out_ref[cut, :] = total.astype(jnp.bfloat16)

    @pl.loop(0, 2 * SUBS)
    def _(index):
        @pl.when(inner | (index < TERMS))
        def _():
            for dest in range(tp_count):
                @pl.when(dest != turn)
                def _():
                    term_copy(right, dest, index).wait_send()

        @pl.when(outer & (index >= TERMS))
        def _():
            ctx_copy(index).wait_send()

    @pl.when(outer)
    def _():
        lend().wait_send()

    @pl.when(inner)
    def _():
        for copy in own_spreads() + [passed_spread(index) for index in range(len(steps))]:
            copy.wait_send()
        if len(straight) < len(steps):
            cross().wait_send()

    each_send(lambda copy: copy.wait_send())
    each_relay(lambda copy: copy.wait_send())


def body(
    tokens, norm_gain, q_weight, q_bias, k_weight, k_bias, v_weight, v_bias, o_weight, doc_ids
):
    rows, model = tokens.shape
    seq_count = lax.axis_size("seq")
    tp_count = lax.axis_size("tp")
    width = q_weight.shape[1]
    cols = o_weight.shape[1] // tp_count
    reach = min(seq_count - 1, (seq_count * rows // 2 + 2 * rows - 2) // rows)
    chunk = rows // 2
    team = math.gcd(seq_count, 8)
    subs = rows // chunk * SUBS
    parts = rows // chunk
    near, far = rope_tables(rows, seq_count)
    hbm = pl.BlockSpec(memory_space=pltpu.HBM)
    vmem = pl.BlockSpec(memory_space=VMEM)
    slots = reach + 1
    spans = -(-width // (2 * HD))
    kdoc = doc_ids.reshape(seq_count, 1, rows)
    return pl.pallas_call(
        functools.partial(attend, seq_count, tp_count, reach, chunk, team),
        out_shape=jax.ShapeDtypeStruct((rows, cols), jnp.bfloat16),
        in_specs=[hbm] * 12,
        out_specs=vmem,
        scratch_shapes=[
            VMEM(norm_gain.shape, jnp.float32),
            VMEM(q_bias.shape, jnp.float32),
            VMEM(k_bias.shape, jnp.float32),
            VMEM(v_bias.shape, jnp.float32),
            VMEM(kdoc.shape, jnp.int32),
            VMEM(far.shape, jnp.float32),
            VMEM((rows, model), jnp.bfloat16),
            VMEM((rows, model), jnp.bfloat16),
            VMEM((model, width), jnp.bfloat16),
            VMEM((model, 2 * HD), jnp.bfloat16),
            VMEM(o_weight.shape, jnp.bfloat16),
            VMEM((2, rows, HD), jnp.float32),
            VMEM((parts, 2 * HD, width // HD * chunk), jnp.bfloat16),
            VMEM((2, rows, HD), jnp.bfloat16),
            VMEM((slots, 2, rows, HD), jnp.bfloat16),
            VMEM((slots, rows, HD), jnp.bfloat16),
            VMEM((HD, width // HD * chunk), jnp.float32),
            VMEM((1, width // HD * chunk), jnp.float32),
            VMEM((1, width // HD * chunk), jnp.float32),
            VMEM((rows, width), jnp.bfloat16),
            VMEM((rows, width), jnp.bfloat16),
            VMEM((width, (tp_count - 1) * cols), jnp.bfloat16),
            VMEM((tp_count, rows, cols), jnp.bfloat16),
            VMEM((2, tp_count, rows, cols), jnp.bfloat16),
            pltpu.SemaphoreType.DMA((14 + spans,)),
            pltpu.SemaphoreType.DMA((slots, 2)),
            pltpu.SemaphoreType.DMA((slots, 2)),
            pltpu.SemaphoreType.DMA((slots, 2)),
            pltpu.SemaphoreType.DMA((2,)),
            pltpu.SemaphoreType.DMA((tp_count, subs)),
            pltpu.SemaphoreType.DMA((2, tp_count, subs)),
            pltpu.SemaphoreType.DMA((subs,)),
            pltpu.SemaphoreType.DMA((subs,)),
            pltpu.SemaphoreType.DMA((2 * team,)),
            pltpu.SemaphoreType.DMA((team,)),
        ],
        compiler_params=pltpu.CompilerParams(
            collective_id=0, has_side_effects=True, vmem_limit_bytes=52 * 1024 * 1024
        ),
    )(
        *[
            pltpu.with_memory_space_constraint(item, pltpu.HBM)
            for item in (
                tokens, norm_gain, q_weight, q_bias, k_weight, k_bias, v_weight, v_bias, o_weight,
                kdoc, jnp.asarray(near), jnp.asarray(far),
            )
        ]
    )


def solution(mesh):
    placed = (
        P("seq", None),
        P(),
        P(None, "tp"),
        P("tp"),
        P(None, "tp"),
        P("tp"),
        P(None, "tp"),
        P("tp"),
        P("tp", None),
        P(),
    )
    return jax.shard_map(
        body, mesh=mesh, in_specs=placed, out_specs=P("seq", "tp"), check_vma=False
    )
```

```python
import functools
import math

import jax
import jax.numpy as jnp
import numpy as np
from jax import lax
from jax.experimental import pallas as pl
from jax.experimental.pallas import tpu as pltpu
from jax.sharding import PartitionSpec as P

HD = 128
MESH = pl.DeviceIdType.MESH
rope_base = 1000000.0
VMEM = pltpu.VMEM
SUBS = 4
TERMS = 5
AHEAD = 3
BACK = 1


def rope_tables(rows, blocks):
    half = HD // 2
    inv = rope_base ** (-(np.arange(half, dtype=np.float64) * 2.0) / HD)
    inv = np.concatenate([inv, inv])[None, :]
    near = np.arange(rows)[:, None] * inv
    far = np.arange(blocks)[:, None] * rows * inv
    near = np.stack([np.cos(near), np.sin(near)]).astype(np.float32)
    far = np.stack([np.cos(far), np.sin(far)])[:, :, None, :].astype(np.float32)
    return near, far


def attend(
    seq_count, tp_count, reach, chunk, team,
    tokens_hbm, gain_hbm, wq_hbm, qb_hbm, wk_hbm, kb_hbm, wv_hbm, vb_hbm, wo_hbm,
    kdoc_hbm, near_hbm, far_hbm, out_ref,
    gain_ref, qb_ref, kb_ref, vb_ref, kdoc_ref, far_ref, tokens, normed, wq, wkv, wo, near, q_ref, kv_ref, kv_in, kext, acc, tops, totals, ctx, ctx_in, lent, sent, got,
    load_sems, kv_send, kv_pass, kv_recv, kv_back, kv_on, send_sem, recv_sem, ctx_send, ctx_recv, lent_send, lent_recv,
):
    place = lax.axis_index("seq")
    turn = lax.axis_index("tp")
    rows, width = tokens.shape[0], wq.shape[1]
    heads = width // HD
    cols = out_ref.shape[1]
    parts = rows // chunk
    factor = math.log2(math.e) / HD**0.5
    step = 2 * HD
    spans = [(lo, min(step, width - lo)) for lo in range(0, width, step)]
    slab = rows // 4
    token_loads = [
        pltpu.make_async_copy(
            tokens_hbm.at[pl.ds(index * slab, slab)], tokens.at[pl.ds(index * slab, slab)],
            load_sems.at[index],
        )
        for index in range(4)
    ]
    near_load = pltpu.make_async_copy(near_hbm, near, load_sems.at[4])
    kv_loads = [
        pltpu.make_async_copy(wk_hbm, wkv.at[:, pl.ds(0, HD)], load_sems.at[5]),
        pltpu.make_async_copy(wv_hbm, wkv.at[:, pl.ds(HD, HD)], load_sems.at[6]),
    ]
    q_loads = [
        pltpu.make_async_copy(
            wq_hbm.at[:, pl.ds(lo, size)], wq.at[:, pl.ds(lo, size)], load_sems.at[7 + index]
        )
        for index, (lo, size) in enumerate(spans)
    ]
    load = pltpu.make_async_copy(wo_hbm, wo, load_sems.at[7 + len(spans)])
    small = [
        pltpu.make_async_copy(source, target, load_sems.at[8 + len(spans) + index])
        for index, (source, target) in enumerate([
            (kdoc_hbm, kdoc_ref), (gain_hbm, gain_ref), (far_hbm, far_ref),
            (kb_hbm, kb_ref), (vb_hbm, vb_ref), (qb_hbm, qb_ref),
        ])
    ]
    for copy in small + token_loads + kv_loads + [near_load]:
        copy.start()

    barrier = pltpu.get_barrier_semaphore()
    span = min(reach + 1, seq_count - 1)
    for away in range(1, span + 1):
        @pl.when(place >= away)
        def _():
            pl.semaphore_signal(barrier, inc=1, device_id={"seq": place - away}, device_id_type=MESH)

        @pl.when(place + away < seq_count)
        def _():
            pl.semaphore_signal(barrier, inc=1, device_id={"seq": place + away}, device_id_type=MESH)

    @pl.when(turn > 0)
    def _():
        pl.semaphore_signal(barrier, inc=1, device_id={"tp": turn - 1}, device_id_type=MESH)

    @pl.when(turn < tp_count - 1)
    def _():
        pl.semaphore_signal(barrier, inc=1, device_id={"tp": turn + 1}, device_id_type=MESH)

    behind = jnp.minimum(place, reach)
    near_count = jnp.minimum(place, span) + jnp.minimum(seq_count - 1 - place, span)
    sides = jnp.where(turn > 0, 1, 0) + jnp.where(turn < tp_count - 1, 1, 0)

    small[0].wait()
    lane = lax.broadcasted_iota(jnp.int32, (rows, HD), 1)
    doc = lax.broadcasted_iota(jnp.int32, (HD, rows), 0)
    for away in range(reach + 1):
        ids = kdoc_ref[jnp.maximum(place - away, 0)]
        kext[away] = jnp.where(doc == ids, 1.0, 0.0).T.astype(jnp.bfloat16)
        if away == 0:
            veto = jnp.where(doc == ids, 0.0, -1e30).astype(jnp.bfloat16)
            for part in range(parts):
                q_ref[part, HD:, :] = jnp.concatenate([veto[:, part * chunk:(part + 1) * chunk]] * heads, axis=1)

    pl.semaphore_wait(barrier, near_count + sides)
    half = tp_count // 2
    right = turn // half
    inner = (turn > 0) & (turn < tp_count - 1)
    outer = jnp.logical_not(inner)
    share = width // team
    mine = lax.rem(place, team)
    base = place - mine
    partner = place + 1 - 2 * lax.rem(place, 2)
    lent_cols = (tp_count - 1) * cols
    steps = list(range(2, team, 2))

    def lend():
        rows_cut = pl.ds(pl.multiple_of(mine * share, 16), share)
        cols_cut = pl.ds(pl.multiple_of((1 - right) * cols, HD), lent_cols)
        return pltpu.make_async_remote_copy(
            src_ref=wo_hbm.at[rows_cut, cols_cut], dst_ref=lent.at[rows_cut],
            send_sem=lent_send.at[0], recv_sem=lent_recv.at[mine],
            device_id={"tp": turn + 1 - 2 * right}, device_id_type=MESH,
        )

    def spread(piece_of, slot, target):
        rows_cut = pl.ds(pl.multiple_of(piece_of * share, 16), share)
        return pltpu.make_async_remote_copy(
            src_ref=lent.at[rows_cut], dst_ref=lent.at[rows_cut],
            send_sem=lent_send.at[slot], recv_sem=lent_recv.at[piece_of],
            device_id={"seq": target}, device_id_type=MESH,
        )

    def mirror(index, bits):
        moved = index
        bit = 1
        while bit < team:
            if bits // bit % 2:
                moved = moved + bit - 2 * bit * lax.rem(index // bit, 2)
            bit *= 2
        return moved

    straight = [bits for bits in steps if bits & (bits - 1) == 0]

    def own_spreads():
        return [spread(mine, 1, partner)] + [
            spread(mine, 2 + index, base + mirror(mine, bits)) for index, bits in enumerate(straight)
        ]

    def passed_spread(index):
        return spread(mirror(mine, steps[index]), 2 + len(steps) + index, partner)

    def cross():
        a, b = mirror(mine, straight[0]), mirror(mine, straight[-1])
        side = lax.rem(mine, 2)
        return spread((1 - side) * a + side * b, 1 + len(steps), base + (1 - side) * b + side * a)

    def hand_over(wanted_steps):
        for index, bits in enumerate(steps):
            if bits in wanted_steps:
                copy = passed_spread(index)
                copy.wait_recv()
                copy.start()

    bent_steps = [bits for bits in steps if bits not in straight]

    def pass_straight():
        hand_over(straight)
        if bent_steps:
            cross().start()

    @pl.when(outer)
    def _():
        lend().start()

    for copy in small[1:]:
        copy.wait()
    gain = gain_ref[...].reshape(1, gain_ref.shape[0])
    for index in range(4):
        token_loads[index].wait()
        if index == 3:
            for copy in q_loads:
                copy.start()

        @pl.loop(0, slab // 64)
        def _(step):
            cut = pl.ds(pl.multiple_of(index * slab + step * 64, 64), 64)
            wide = tokens[cut, :].astype(jnp.float32)
            mean = jnp.mean(wide * wide, axis=-1, keepdims=True)
            normed[cut, :] = (wide * lax.rsqrt(mean + 1e-06) * gain).astype(jnp.bfloat16)

    near_load.wait()
    far_cos, far_sin = far_ref[0, place], far_ref[1, place]
    cos = near[0] * far_cos - near[1] * far_sin
    sin = near[1] * far_cos + near[0] * far_sin
    near[0] = cos
    near[1] = jnp.where(lane < HD // 2, -sin, sin)

    def rope(t):
        return t * near[0] + pltpu.roll(t, HD // 2, 1) * near[1]

    for copy in kv_loads:
        copy.wait()
    kv = jnp.dot(normed[...], wkv[...], preferred_element_type=jnp.float32)
    kv_ref[0] = rope(kv[:, :HD] + kb_ref[...].reshape(1, HD)).astype(jnp.bfloat16)
    values = kv[:, HD:] + vb_ref[...].reshape(1, HD)
    for lo in range(0, rows, HD):
        kv_ref[1, lo:lo + HD] = values[lo:lo + HD].T.astype(jnp.bfloat16)

    odd = lax.rem(place, 2) == 1

    core = lax.rem(place, 2)
    bent = lax.rem(place // 2, 2) == 1
    bends = reach >= 4

    def kv_cut(ref, part):
        if part == 0:
            return ref.at[0]
        return ref.at[1, pl.ds((part - 1) * (rows // 2), rows // 2)]

    def kv_copy(away, part):
        return pltpu.make_async_remote_copy(
            src_ref=kv_cut(kv_ref, part), dst_ref=kv_cut(kv_in.at[away - 1], part),
            send_sem=kv_send.at[away // 2, part], recv_sem=kv_recv.at[away - 1, part],
            device_id={"seq": lax.rem(place + away, seq_count)}, device_id_type=MESH,
        )

    def relay(away, landing, part):
        return pltpu.make_async_remote_copy(
            src_ref=kv_cut(kv_in.at[away - 1], part), dst_ref=kv_cut(kv_in.at[landing - 1], part),
            send_sem=kv_pass.at[away // 2 - 1, part], recv_sem=kv_recv.at[landing - 1, part],
            device_id={"seq": partner}, device_id_type=MESH,
        )

    def back(part):
        return pltpu.make_async_remote_copy(
            src_ref=kv_cut(kv_in.at[3], part), dst_ref=kv_cut(kv_in.at[1], part),
            send_sem=kv_back.at[part], recv_sem=kv_recv.at[1, part],
            device_id={"seq": lax.rem(place + seq_count - 2, seq_count)}, device_id_type=MESH,
        )

    pieces = (0, 1, 2)
    evens = [away for away in range(2, reach + 2, 2) if away < seq_count]
    backs = bent & (place >= 4) & bends
    beyond = bool(evens) and evens[-1] > reach and evens[-1] > 2

    def onward(part):
        return pltpu.make_async_remote_copy(
            src_ref=kv_cut(kv_in.at[evens[-2] - 1], part), dst_ref=kv_cut(kv_in.at[evens[-1] - 1], part),
            send_sem=kv_on.at[part], recv_sem=kv_recv.at[evens[-1] - 1, part],
            device_id={"seq": lax.rem(place + 2, seq_count)}, device_id_type=MESH,
        )

    def carries(away):
        return odd & (place >= away) & (place + 2 < seq_count)

    def wanted(away):
        return odd if away > reach else (place >= 0)

    def each_send(act):
        for part in pieces:
            for away in evens:
                direct = jnp.logical_not(bent & (place + 4 < seq_count) & bends & (away == 2))

                if not (beyond and away > reach):
                    @pl.when((place + away < seq_count) & wanted(away) & direct)
                    def _():
                        act(kv_copy(away, part))

            @pl.when(jnp.logical_not(odd))
            def _():
                act(kv_copy(1, part))

    def each_relay(act):
        for part in pieces:
            for away in evens:
                if away + 1 <= reach:
                    @pl.when((place >= away) & jnp.logical_not(odd))
                    def _():
                        act(relay(away, away + 1, part))

                @pl.when((place >= away) & odd)
                def _():
                    act(relay(away, away - 1, part))

            if bends:
                @pl.when(backs)
                def _():
                    act(back(part))

            if beyond:
                @pl.when(carries(evens[-2]))
                def _():
                    act(onward(part))

    def take(group):
        for part in pieces:
            @pl.when(jnp.logical_not(backs & (group == 4)))
            def _():
                kv_copy(group, part).wait_recv()

            @pl.when(odd | (group + 1 <= reach))
            def _():
                relay(group, group + 1 - 2 * core, part).start()

        if beyond:
            @pl.when(carries(evens[-2]) & (group == evens[-2]))
            def _():
                for part in pieces:
                    onward(part).start()

    def obtain(away):
        even = lax.rem(away, 2) == 0

        @pl.when(even & (jnp.logical_not(odd) | (away == behind)))
        def _():
            take(away)

        @pl.when(jnp.logical_not(even) & odd & (away > 2))
        def _():
            take(away - 1)

        if evens and evens[-1] > reach:
            @pl.when((away == 2) & odd & (place >= evens[-1]))
            def _():
                take(evens[-1])

        @pl.when(jnp.logical_not(even))
        def _():
            for part in pieces:
                kv_copy(away, part).wait_recv()

    def bounce(part):
        if bends:
            @pl.when(backs)
            def _():
                kv_copy(4, part).wait_recv()
                back(part).start()

    each_send(lambda copy: copy.start())

    for index in range(0, len(spans), 2):
        for copy in q_loads[index:index + 2]:
            copy.wait()
        if index == 0:
            load.start()
        lo = spans[index][0]
        size = sum(extent for _, extent in spans[index:index + 2])
        out = jnp.dot(
            normed[...], wq[:, lo:lo + size], preferred_element_type=jnp.float32
        ) + qb_ref[lo:lo + size].reshape(1, size)
        for head in range(0, size, HD):
            turned = rope(out[:, head:head + HD]) * factor
            at = (lo + head) // HD * chunk
            for part in range(parts):
                q_ref[part, :HD, at:at + chunk] = turned[part * chunk:(part + 1) * chunk].T.astype(jnp.bfloat16)

    def offer():
        spread(mine, 1, partner).wait_recv()
        for copy in own_spreads():
            copy.start()

    sub = chunk // SUBS

    def sub_cut(index):
        return pl.ds(pl.multiple_of(index * sub, sub), sub)

    def arrival(side, dest, index, taker):
        half_of = taker // half
        outward = lax.rem(side + half_of, 2)
        near = (1 - half_of) * dest + half_of * (tp_count - 1 - dest)
        first = (tp_count - 1 - near) * TERMS
        second = (tp_count - 1) * TERMS + near * 2 * SUBS
        return (1 - outward) * first + outward * second + index

    def term_copy(side, dest, index):
        return pltpu.make_async_remote_copy(
            src_ref=sent.at[dest, sub_cut(index)], dst_ref=got.at[side, dest, sub_cut(index)],
            send_sem=send_sem.at[lax.rem(dest - turn - 1 + tp_count, tp_count), index],
            recv_sem=recv_sem.at[arrival(side, dest, index, turn + 1 - 2 * side)],
            device_id={"tp": turn + 1 - 2 * side}, device_id_type=MESH,
        )

    def term_wait(side, dest, index):
        pltpu.make_async_remote_copy(
            src_ref=sent.at[dest, sub_cut(index)], dst_ref=got.at[side, dest, sub_cut(index)],
            send_sem=send_sem.at[0, index], recv_sem=recv_sem.at[arrival(side, dest, index, turn)],
            device_id={"tp": turn + 1 - 2 * side}, device_id_type=MESH,
        ).wait_recv()

    def ctx_copy(index):
        return pltpu.make_async_remote_copy(
            src_ref=ctx.at[sub_cut(index)], dst_ref=ctx_in.at[sub_cut(index)],
            send_sem=ctx_send.at[index - TERMS], recv_sem=ctx_recv.at[index - TERMS],
            device_id={"tp": turn + 1 - 2 * right}, device_id_type=MESH,
        )

    last = tp_count - 1
    far = (1 - right) * last
    home = right * last
    farther = (1 - right) * (last - 1) + right
    other = turn + 1 - 2 * lax.rem(turn, 2)

    def forward(side, dest, index):
        cut = sub_cut(index)
        term_wait(side, dest, index)
        sent[dest, cut] = (
            sent[dest, cut].astype(jnp.float32) + got[side, dest, cut].astype(jnp.float32)
        ).astype(jnp.bfloat16)
        term_copy(side, dest, index).start()

    def event(index):
        @pl.when(index < 2 * SUBS)
        def _():
            forward(right, far + index // SUBS * (farther - far), lax.rem(index, SUBS))

        @pl.when((index > 1) & (index < SUBS + 2))
        def _():
            forward(1 - right, home, index - 2)

    wide = step // chunk * chunk
    tiles = [(lo, min(wide, heads * chunk - lo)) for lo in range(0, heads * chunk, wide)]

    def piece(part):
        cut = pl.ds(pl.multiple_of(part * chunk, chunk), chunk)
        def block(held, away, first):
            keys = jnp.concatenate([held[0], kext[away]], axis=1)
            values = jnp.concatenate([held[1, lo:lo + HD] for lo in range(0, rows, HD)], axis=1)
            if first:
                key = lax.broadcasted_iota(jnp.int32, (rows, chunk), 0)
                row = part * chunk + lax.broadcasted_iota(jnp.int32, (rows, chunk), 1)
                later = jnp.where(key <= row, 0.0, -1e30)
            def score(tile):
                lo, size = tile
                s = jnp.dot(keys, q_ref[part, :, lo:lo + size], preferred_element_type=jnp.float32)
                if first:
                    s = s + jnp.concatenate([later] * (size // chunk), axis=1)
                return s

            def weigh(tile, s):
                lo, size = tile
                fresh = jnp.max(s, axis=0, keepdims=True)
                scale = None
                if not first:
                    top = tops[:, lo:lo + size]
                    fresh = jnp.maximum(top, fresh)
                    scale = jnp.exp2(top - fresh)
                e = jnp.exp2(s - fresh)
                total = jnp.sum(e, axis=0, keepdims=True)
                if not first:
                    total = total + totals[:, lo:lo + size] * scale
                tops[:, lo:lo + size] = fresh
                totals[:, lo:lo + size] = total
                return tile, scale, e.astype(jnp.bfloat16)

            def mix(tile, scale, e):
                return tile, scale, jnp.dot(values, e, preferred_element_type=jnp.float32)

            def gather(tile, scale, pv):
                lo, size = tile
                if not first:
                    pv = pv + acc[:, lo:lo + size] * scale
                acc[:, lo:lo + size] = pv

            ready = [score(tile) for tile in tiles[:AHEAD]]
            mixed = []
            for index, tile in enumerate(tiles):
                if index + AHEAD < len(tiles):
                    ready.append(score(tiles[index + AHEAD]))
                mixed.append(mix(*weigh(tile, ready.pop(0))))
                if len(mixed) > BACK:
                    gather(*mixed.pop(0))
            while mixed:
                gather(*mixed.pop(0))

        @pl.when(part == 0)
        def _():
            bounce(0)

        block(kv_ref, 0, True)
        @pl.when(part == 0)
        def _():
            bounce(1)
            bounce(2)

        tail = (1 - core) * (behind // reach) * (reach % 2) if reach else 0

        @pl.loop(1, behind + 1)
        def _(turned):
            away = lax.rem(2 * behind - turned - tail + core, behind) + 1

            @pl.when(part == 0)
            def _():
                obtain(away)

            @pl.when((part == 0) & inner & (behind > 1) & (turned == behind))
            def _():
                offer()

            @pl.when((part == 1) & inner)
            def _():
                event(turned - 1)

            @pl.when((part == 1) & inner & (turned == behind - 1) & (behind > 4))
            def _():
                pass_straight()

            block(kv_in.at[away - 1], away, False)

        whole = acc[...] * (1.0 / totals[...])
        context = jnp.concatenate(
            [whole[:, h * chunk:(h + 1) * chunk].T.astype(jnp.bfloat16) for h in range(heads)], axis=1
        )
        ctx[cut, :] = context

        @pl.when((part == 1) & inner)
        def _():
            event(behind)

            @pl.when((behind > 1) & (behind < 5))
            def _():
                pass_straight()

        @pl.when(part == 0)
        def _():
            load.wait()

        def term(dest):
            sent[dest, cut] = jnp.dot(
                context, wo[:, pl.ds(pl.multiple_of(dest * cols, HD), cols)],
                preferred_element_type=jnp.float32,
            ).astype(jnp.bfloat16)

        def launch(dest):
            @pl.when((part == 0) & outer)
            def _():
                for index in range(SUBS):
                    term_copy(right, dest, index).start()

            @pl.when((part == 1) & outer)
            def _():
                for index in range(SUBS, TERMS):
                    term_copy(right, dest, index).start()

        term(far)
        launch(far)
        term(farther)
        launch(farther)

        @pl.when((part == 1) & outer)
        def _():
            for index in range(TERMS, 2 * SUBS):
                ctx_copy(index).start()
            for index in range(SUBS):
                term_copy(right, other, index).start()

        term(other)
        term(turn)

        @pl.when((part == 1) & outer)
        def _():
            for index in range(SUBS, TERMS):
                term_copy(right, other, index).start()

        @pl.when((part == 0) & inner & (behind < 2))
        def _():
            offer()

    @pl.loop(0, 2)
    def _(part):
        piece(part)

    @pl.when(inner)
    def _():
        split = jnp.where(behind > 1, behind + 1, 2 * SUBS - 1)
        early = (behind > 4) & (behind < 2 * SUBS - 2)

        @pl.loop(behind + 1, split)
        def _(index):
            event(index)

        @pl.when(behind < 2)
        def _():
            pass_straight()

        @pl.loop(split, 2 * SUBS)
        def _(index):
            event(index)

            @pl.when((index == 2 * SUBS - 2) & early)
            def _():
                hand_over(bent_steps)

        for index in range(SUBS, TERMS):
            forward(right, far, index)
            forward(right, farther, index)

        @pl.when(jnp.logical_not(early))
        def _():
            hand_over(bent_steps)

        twin = mine + 1 - 2 * lax.rem(mine, 2)
        for bits in [0] + steps:
            spread(mirror(twin, bits), 1, partner).wait_recv()

        @pl.loop(TERMS, 2 * SUBS)
        def _(index):
            cut = sub_cut(index)
            ctx_copy(index).wait_recv()
            guest = ctx_in[cut, :]
            for at in range(tp_count - 1):
                dest = at + 1 - right
                sent[dest, cut] = (
                    sent[dest, cut].astype(jnp.float32)
                    + jnp.dot(
                        guest, lent[:, at * cols:(at + 1) * cols], preferred_element_type=jnp.float32
                    )
                ).astype(jnp.bfloat16)
            term_copy(right, far, index).start()

        for index in range(TERMS, 2 * SUBS):
            term_copy(right, farther, index).start()
        for index in range(SUBS, 2 * SUBS):
            forward(1 - right, home, index)

    @pl.when(outer)
    def _():
        lend().wait_send()

    @pl.when(inner)
    def _():
        for copy in own_spreads() + [passed_spread(index) for index in range(len(steps))]:
            copy.wait_send()
        if bent_steps:
            cross().wait_send()

    each_send(lambda copy: copy.wait_send())
    each_relay(lambda copy: copy.wait_send())

    def finish(index):
        cut = sub_cut(index)
        term_wait(1 - right, turn, index)
        total = sent[turn, cut].astype(jnp.float32) + got[1 - right, turn, cut].astype(jnp.float32)
        both = inner & (index < TERMS)

        @pl.when(both)
        def _():
            term_wait(right, turn, index)
            out_ref[cut, :] = (total + got[right, turn, cut].astype(jnp.float32)).astype(jnp.bfloat16)

        @pl.when(jnp.logical_not(both))
        def _():
            out_ref[cut, :] = total.astype(jnp.bfloat16)

    @pl.loop(0, 2 * SUBS - 1)
    def _(index):
        finish(index)

    @pl.loop(0, 2 * SUBS)
    def _(index):
        @pl.when(inner | (index < TERMS))
        def _():
            for ahead in range(1, tp_count):
                term_copy(right, lax.rem(turn + ahead, tp_count), index).wait_send()

        @pl.when(outer & (index >= TERMS))
        def _():
            ctx_copy(index).wait_send()

    finish(2 * SUBS - 1)


def body(
    tokens, norm_gain, q_weight, q_bias, k_weight, k_bias, v_weight, v_bias, o_weight, doc_ids
):
    rows, model = tokens.shape
    seq_count = lax.axis_size("seq")
    tp_count = lax.axis_size("tp")
    width = q_weight.shape[1]
    cols = o_weight.shape[1] // tp_count
    reach = min(seq_count - 1, (seq_count * rows // 2 + 2 * rows - 2) // rows)
    chunk = rows // 2
    team = math.gcd(seq_count, 8)
    subs = rows // chunk * SUBS
    parts = rows // chunk
    near, far = rope_tables(rows, seq_count)
    hbm = pl.BlockSpec(memory_space=pltpu.HBM)
    vmem = pl.BlockSpec(memory_space=VMEM)
    slots = reach + 1
    spans = -(-width // (2 * HD))
    kdoc = doc_ids.reshape(seq_count, 1, rows)
    return pl.pallas_call(
        functools.partial(attend, seq_count, tp_count, reach, chunk, team),
        out_shape=jax.ShapeDtypeStruct((rows, cols), jnp.bfloat16),
        in_specs=[hbm] * 12,
        out_specs=vmem,
        scratch_shapes=[
            VMEM(norm_gain.shape, jnp.float32),
            VMEM(q_bias.shape, jnp.float32),
            VMEM(k_bias.shape, jnp.float32),
            VMEM(v_bias.shape, jnp.float32),
            VMEM(kdoc.shape, jnp.int32),
            VMEM(far.shape, jnp.float32),
            VMEM((rows, model), jnp.bfloat16),
            VMEM((rows, model), jnp.bfloat16),
            VMEM((model, width), jnp.bfloat16),
            VMEM((model, 2 * HD), jnp.bfloat16),
            VMEM(o_weight.shape, jnp.bfloat16),
            VMEM((2, rows, HD), jnp.float32),
            VMEM((parts, 2 * HD, width // HD * chunk), jnp.bfloat16),
            VMEM((2, rows, HD), jnp.bfloat16),
            VMEM((slots, 2, rows, HD), jnp.bfloat16),
            VMEM((slots, rows, HD), jnp.bfloat16),
            VMEM((HD, width // HD * chunk), jnp.float32),
            VMEM((1, width // HD * chunk), jnp.float32),
            VMEM((1, width // HD * chunk), jnp.float32),
            VMEM((rows, width), jnp.bfloat16),
            VMEM((rows, width), jnp.bfloat16),
            VMEM((width, (tp_count - 1) * cols), jnp.bfloat16),
            VMEM((tp_count, rows, cols), jnp.bfloat16),
            VMEM((2, tp_count, rows, cols), jnp.bfloat16),
            pltpu.SemaphoreType.DMA((14 + spans,)),
            pltpu.SemaphoreType.DMA((slots // 2 + 1, 3)),
            pltpu.SemaphoreType.DMA((max(slots // 2, 1), 3)),
            pltpu.SemaphoreType.DMA((slots, 3)),
            pltpu.SemaphoreType.DMA((3,)),
            pltpu.SemaphoreType.DMA((3,)),
            pltpu.SemaphoreType.DMA((tp_count - 1, subs)),
            pltpu.SemaphoreType.DMA(((tp_count - 1) * TERMS + 2 * subs,)),
            pltpu.SemaphoreType.DMA((subs - TERMS,)),
            pltpu.SemaphoreType.DMA((subs - TERMS,)),
            pltpu.SemaphoreType.DMA((team,)),
            pltpu.SemaphoreType.DMA((team,)),
        ],
        compiler_params=pltpu.CompilerParams(
            collective_id=0, has_side_effects=True, vmem_limit_bytes=52 * 1024 * 1024
        ),
    )(
        *[
            pltpu.with_memory_space_constraint(item, pltpu.HBM)
            for item in (
                tokens, norm_gain, q_weight, q_bias, k_weight, k_bias, v_weight, v_bias, o_weight,
                kdoc, jnp.asarray(near), jnp.asarray(far),
            )
        ]
    )


def solution(mesh):
    placed = (
        P("seq", None),
        P(),
        P(None, "tp"),
        P("tp"),
        P(None, "tp"),
        P("tp"),
        P(None, "tp"),
        P("tp"),
        P("tp", None),
        P(),
    )
    return jax.shard_map(
        body, mesh=mesh, in_specs=placed, out_specs=P("seq", "tp"), check_vma=False
    )
```

```python
import functools
import math

import jax
import jax.numpy as jnp
import numpy as np
from jax import lax
from jax.experimental import pallas as pl
from jax.experimental.pallas import tpu as pltpu
from jax.sharding import PartitionSpec as P

HD = 128
MESH = pl.DeviceIdType.MESH
rope_base = 1000000.0
VMEM = pltpu.VMEM
SUBS = 4
TERMS = 4
AHEAD = 3
BACK = 1


def rope_tables(rows, blocks):
    half = HD // 2
    inv = rope_base ** (-(np.arange(half, dtype=np.float64) * 2.0) / HD)
    inv = np.concatenate([inv, inv])[None, :]
    near = np.arange(rows)[:, None] * inv
    far = np.arange(blocks)[:, None] * rows * inv
    near = np.stack([np.cos(near), np.sin(near)]).astype(np.float32)
    far = np.stack([np.cos(far), np.sin(far)])[:, :, None, :].astype(np.float32)
    return near, far


def attend(
    seq_count, tp_count, reach, chunk, team,
    tokens_hbm, gain_hbm, wq_hbm, qb_hbm, wk_hbm, kb_hbm, wv_hbm, vb_hbm, wo_hbm,
    kdoc_hbm, near_hbm, far_hbm, out_ref,
    gain_ref, qb_ref, kb_ref, vb_ref, kdoc_ref, far_ref, tokens, normed, wq, wkv, wo, near, q_ref, kv_ref, kv_in, kext, acc, tops, totals, ctx, ctx_in, lent, sent, got,
    load_sems, kv_send, kv_pass, kv_recv, kv_back, kv_on, send_sem, recv_sem, ctx_send, ctx_recv, lent_send, lent_recv,
):
    place = lax.axis_index("seq")
    turn = lax.axis_index("tp")
    rows, width = tokens.shape[0], wq.shape[1]
    heads = width // HD
    cols = out_ref.shape[1]
    parts = rows // chunk
    factor = math.log2(math.e) / HD**0.5
    step = 2 * HD
    spans = [(lo, min(step, width - lo)) for lo in range(0, width, step)]
    slab = rows // 4
    token_loads = [
        pltpu.make_async_copy(
            tokens_hbm.at[pl.ds(index * slab, slab)], tokens.at[pl.ds(index * slab, slab)],
            load_sems.at[index],
        )
        for index in range(4)
    ]
    near_load = pltpu.make_async_copy(near_hbm, near, load_sems.at[4])
    kv_loads = [
        pltpu.make_async_copy(wk_hbm, wkv.at[:, pl.ds(0, HD)], load_sems.at[5]),
        pltpu.make_async_copy(wv_hbm, wkv.at[:, pl.ds(HD, HD)], load_sems.at[6]),
    ]
    q_loads = [
        pltpu.make_async_copy(
            wq_hbm.at[:, pl.ds(lo, size)], wq.at[:, pl.ds(lo, size)], load_sems.at[7 + index]
        )
        for index, (lo, size) in enumerate(spans)
    ]
    load = pltpu.make_async_copy(wo_hbm, wo, load_sems.at[7 + len(spans)])
    small = [
        pltpu.make_async_copy(source, target, load_sems.at[8 + len(spans) + index])
        for index, (source, target) in enumerate([
            (kdoc_hbm, kdoc_ref), (gain_hbm, gain_ref), (far_hbm, far_ref),
            (kb_hbm, kb_ref), (vb_hbm, vb_ref), (qb_hbm, qb_ref),
        ])
    ]
    for copy in small + token_loads + kv_loads + [near_load]:
        copy.start()

    barrier = pltpu.get_barrier_semaphore()
    span = min(reach + 1, seq_count - 1)
    for away in range(1, span + 1):
        @pl.when(place >= away)
        def _():
            pl.semaphore_signal(barrier, inc=1, device_id={"seq": place - away}, device_id_type=MESH)

        @pl.when(place + away < seq_count)
        def _():
            pl.semaphore_signal(barrier, inc=1, device_id={"seq": place + away}, device_id_type=MESH)

    @pl.when(turn > 0)
    def _():
        pl.semaphore_signal(barrier, inc=1, device_id={"tp": turn - 1}, device_id_type=MESH)

    @pl.when(turn < tp_count - 1)
    def _():
        pl.semaphore_signal(barrier, inc=1, device_id={"tp": turn + 1}, device_id_type=MESH)

    behind = jnp.minimum(place, reach)
    near_count = jnp.minimum(place, span) + jnp.minimum(seq_count - 1 - place, span)
    sides = jnp.where(turn > 0, 1, 0) + jnp.where(turn < tp_count - 1, 1, 0)

    small[0].wait()
    lane = lax.broadcasted_iota(jnp.int32, (rows, HD), 1)
    doc = lax.broadcasted_iota(jnp.int32, (HD, rows), 0)
    for away in range(reach + 1):
        ids = kdoc_ref[jnp.maximum(place - away, 0)]
        kext[away] = jnp.where(doc == ids, 1.0, 0.0).T.astype(jnp.bfloat16)
        if away == 0:
            veto = jnp.where(doc == ids, 0.0, -1e30).astype(jnp.bfloat16)
            for part in range(parts):
                q_ref[part, HD:, :] = jnp.concatenate([veto[:, part * chunk:(part + 1) * chunk]] * heads, axis=1)

    pl.semaphore_wait(barrier, near_count + sides)
    half = tp_count // 2
    right = turn // half
    inner = (turn > 0) & (turn < tp_count - 1)
    outer = jnp.logical_not(inner)
    share = width // team
    mine = lax.rem(place, team)
    base = place - mine
    partner = place + 1 - 2 * lax.rem(place, 2)
    lent_cols = (tp_count - 1) * cols
    steps = list(range(2, team, 2))

    def lend():
        rows_cut = pl.ds(pl.multiple_of(mine * share, 16), share)
        cols_cut = pl.ds(pl.multiple_of((1 - right) * cols, HD), lent_cols)
        return pltpu.make_async_remote_copy(
            src_ref=wo_hbm.at[rows_cut, cols_cut], dst_ref=lent.at[rows_cut],
            send_sem=lent_send.at[0], recv_sem=lent_recv.at[mine],
            device_id={"tp": turn + 1 - 2 * right}, device_id_type=MESH,
        )

    def spread(piece_of, slot, target):
        rows_cut = pl.ds(pl.multiple_of(piece_of * share, 16), share)
        return pltpu.make_async_remote_copy(
            src_ref=lent.at[rows_cut], dst_ref=lent.at[rows_cut],
            send_sem=lent_send.at[slot], recv_sem=lent_recv.at[piece_of],
            device_id={"seq": target}, device_id_type=MESH,
        )

    def mirror(index, bits):
        moved = index
        bit = 1
        while bit < team:
            if bits // bit % 2:
                moved = moved + bit - 2 * bit * lax.rem(index // bit, 2)
            bit *= 2
        return moved

    straight = [bits for bits in steps if bits & (bits - 1) == 0]

    def own_spreads():
        return [spread(mine, 1, partner)] + [
            spread(mine, 2 + index, base + mirror(mine, bits)) for index, bits in enumerate(straight)
        ]

    def passed_spread(index):
        return spread(mirror(mine, steps[index]), 2 + len(steps) + index, partner)

    def cross():
        a, b = mirror(mine, straight[0]), mirror(mine, straight[-1])
        side = lax.rem(mine, 2)
        return spread((1 - side) * a + side * b, 1 + len(steps), base + (1 - side) * b + side * a)

    def hand_over(wanted_steps):
        for index, bits in enumerate(steps):
            if bits in wanted_steps:
                copy = passed_spread(index)
                copy.wait_recv()
                copy.start()

    bent_steps = [bits for bits in steps if bits not in straight]

    def pass_straight():
        hand_over(straight)
        if bent_steps:
            cross().start()

    @pl.when(outer)
    def _():
        lend().start()

    for copy in small[1:]:
        copy.wait()
    gain = gain_ref[...].reshape(1, gain_ref.shape[0])
    for index in range(4):
        token_loads[index].wait()
        if index == 3:
            for copy in q_loads:
                copy.start()

        @pl.loop(0, slab // 64)
        def _(step):
            cut = pl.ds(pl.multiple_of(index * slab + step * 64, 64), 64)
            wide = tokens[cut, :].astype(jnp.float32)
            mean = jnp.mean(wide * wide, axis=-1, keepdims=True)
            normed[cut, :] = (wide * lax.rsqrt(mean + 1e-06) * gain).astype(jnp.bfloat16)

    near_load.wait()
    far_cos, far_sin = far_ref[0, place], far_ref[1, place]
    cos = near[0] * far_cos - near[1] * far_sin
    sin = near[1] * far_cos + near[0] * far_sin
    near[0] = cos
    near[1] = jnp.where(lane < HD // 2, -sin, sin)

    def rope(t):
        return t * near[0] + pltpu.roll(t, HD // 2, 1) * near[1]

    for copy in kv_loads:
        copy.wait()
    kv = jnp.dot(normed[...], wkv[...], preferred_element_type=jnp.float32)
    kv_ref[0] = rope(kv[:, :HD] + kb_ref[...].reshape(1, HD)).astype(jnp.bfloat16)
    values = kv[:, HD:] + vb_ref[...].reshape(1, HD)
    for lo in range(0, rows, HD):
        kv_ref[1, lo:lo + HD] = values[lo:lo + HD].T.astype(jnp.bfloat16)

    odd = lax.rem(place, 2) == 1

    core = lax.rem(place, 2)
    bent = lax.rem(place // 2, 2) == 1
    bends = reach >= 4

    def kv_cut(ref, part):
        if part == 0:
            return ref.at[0]
        return ref.at[1, pl.ds((part - 1) * (rows // 2), rows // 2)]

    def kv_copy(away, part):
        return pltpu.make_async_remote_copy(
            src_ref=kv_cut(kv_ref, part), dst_ref=kv_cut(kv_in.at[away - 1], part),
            send_sem=kv_send.at[away // 2, part], recv_sem=kv_recv.at[away - 1, part],
            device_id={"seq": lax.rem(place + away, seq_count)}, device_id_type=MESH,
        )

    def relay(away, landing, part):
        return pltpu.make_async_remote_copy(
            src_ref=kv_cut(kv_in.at[away - 1], part), dst_ref=kv_cut(kv_in.at[landing - 1], part),
            send_sem=kv_pass.at[away // 2 - 1, part], recv_sem=kv_recv.at[landing - 1, part],
            device_id={"seq": partner}, device_id_type=MESH,
        )

    def back(part):
        return pltpu.make_async_remote_copy(
            src_ref=kv_cut(kv_in.at[3], part), dst_ref=kv_cut(kv_in.at[1], part),
            send_sem=kv_back.at[part], recv_sem=kv_recv.at[1, part],
            device_id={"seq": lax.rem(place + seq_count - 2, seq_count)}, device_id_type=MESH,
        )

    pieces = (0, 1, 2)
    evens = [away for away in range(2, reach + 2, 2) if away < seq_count]
    backs = bent & (place >= 4) & bends
    beyond = bool(evens) and evens[-1] > reach and evens[-1] > 2

    def onward(part):
        return pltpu.make_async_remote_copy(
            src_ref=kv_cut(kv_in.at[evens[-2] - 1], part), dst_ref=kv_cut(kv_in.at[evens[-1] - 1], part),
            send_sem=kv_on.at[part], recv_sem=kv_recv.at[evens[-1] - 1, part],
            device_id={"seq": lax.rem(place + 2, seq_count)}, device_id_type=MESH,
        )

    def carries(away):
        return odd & (place >= away) & (place + 2 < seq_count)

    def wanted(away):
        return odd if away > reach else (place >= 0)

    def each_send(act):
        for part in pieces:
            for away in evens:
                direct = jnp.logical_not(bent & (place + 4 < seq_count) & bends & (away == 2))

                if not (beyond and away > reach):
                    @pl.when((place + away < seq_count) & wanted(away) & direct)
                    def _():
                        act(kv_copy(away, part))

            @pl.when(jnp.logical_not(odd))
            def _():
                act(kv_copy(1, part))

    def each_relay(act):
        for part in pieces:
            for away in evens:
                if away + 1 <= reach:
                    @pl.when((place >= away) & jnp.logical_not(odd))
                    def _():
                        act(relay(away, away + 1, part))

                @pl.when((place >= away) & odd)
                def _():
                    act(relay(away, away - 1, part))

            if bends:
                @pl.when(backs)
                def _():
                    act(back(part))

            if beyond:
                @pl.when(carries(evens[-2]))
                def _():
                    act(onward(part))

    def take(group):
        for part in pieces:
            @pl.when(jnp.logical_not(backs & (group == 4)))
            def _():
                kv_copy(group, part).wait_recv()

            @pl.when(odd | (group + 1 <= reach))
            def _():
                relay(group, group + 1 - 2 * core, part).start()

        if beyond:
            @pl.when(carries(evens[-2]) & (group == evens[-2]))
            def _():
                for part in pieces:
                    onward(part).start()

    def obtain(away):
        even = lax.rem(away, 2) == 0

        @pl.when(even & (jnp.logical_not(odd) | (away == behind)))
        def _():
            take(away)

        @pl.when(jnp.logical_not(even) & odd & (away > 2))
        def _():
            take(away - 1)

        if evens and evens[-1] > reach:
            @pl.when((away == 2) & odd & (place >= evens[-1]))
            def _():
                take(evens[-1])

        @pl.when(jnp.logical_not(even))
        def _():
            for part in pieces:
                kv_copy(away, part).wait_recv()

    def bounce(part):
        if bends:
            @pl.when(backs)
            def _():
                kv_copy(4, part).wait_recv()
                back(part).start()

    each_send(lambda copy: copy.start())

    for index in range(0, len(spans), 2):
        for copy in q_loads[index:index + 2]:
            copy.wait()
        if index == 0:
            load.start()
        lo = spans[index][0]
        size = sum(extent for _, extent in spans[index:index + 2])
        out = jnp.dot(
            normed[...], wq[:, lo:lo + size], preferred_element_type=jnp.float32
        ) + qb_ref[lo:lo + size].reshape(1, size)
        for head in range(0, size, HD):
            turned = rope(out[:, head:head + HD]) * factor
            at = (lo + head) // HD * chunk
            for part in range(parts):
                q_ref[part, :HD, at:at + chunk] = turned[part * chunk:(part + 1) * chunk].T.astype(jnp.bfloat16)

    def offer():
        spread(mine, 1, partner).wait_recv()
        for copy in own_spreads():
            copy.start()

    sub = chunk // SUBS

    def sub_cut(index):
        return pl.ds(pl.multiple_of(index * sub, sub), sub)

    def arrival(side, dest, index, taker):
        half_of = taker // half
        outward = lax.rem(side + half_of, 2)
        near = (1 - half_of) * dest + half_of * (tp_count - 1 - dest)
        first = (tp_count - 1 - near) * TERMS
        second = (tp_count - 1) * TERMS + near * 2 * SUBS
        return (1 - outward) * first + outward * second + index

    def term_copy(side, dest, index):
        return pltpu.make_async_remote_copy(
            src_ref=sent.at[dest, sub_cut(index)], dst_ref=got.at[side, dest, sub_cut(index)],
            send_sem=send_sem.at[lax.rem(dest - turn - 1 + tp_count, tp_count), index],
            recv_sem=recv_sem.at[arrival(side, dest, index, turn + 1 - 2 * side)],
            device_id={"tp": turn + 1 - 2 * side}, device_id_type=MESH,
        )

    def term_wait(side, dest, index):
        pltpu.make_async_remote_copy(
            src_ref=sent.at[dest, sub_cut(index)], dst_ref=got.at[side, dest, sub_cut(index)],
            send_sem=send_sem.at[0, index], recv_sem=recv_sem.at[arrival(side, dest, index, turn)],
            device_id={"tp": turn + 1 - 2 * side}, device_id_type=MESH,
        ).wait_recv()

    def ctx_copy(index):
        return pltpu.make_async_remote_copy(
            src_ref=ctx.at[sub_cut(index)], dst_ref=ctx_in.at[sub_cut(index)],
            send_sem=ctx_send.at[index - TERMS], recv_sem=ctx_recv.at[index - TERMS],
            device_id={"tp": turn + 1 - 2 * right}, device_id_type=MESH,
        )

    last = tp_count - 1
    far = (1 - right) * last
    home = right * last
    farther = (1 - right) * (last - 1) + right
    other = turn + 1 - 2 * lax.rem(turn, 2)

    def forward(side, dest, index):
        cut = sub_cut(index)
        term_wait(side, dest, index)
        sent[dest, cut] = (
            sent[dest, cut].astype(jnp.float32) + got[side, dest, cut].astype(jnp.float32)
        ).astype(jnp.bfloat16)
        term_copy(side, dest, index).start()

    def event(index):
        @pl.when(index < 2 * SUBS)
        def _():
            forward(right, far + index // SUBS * (farther - far), lax.rem(index, SUBS))

        @pl.when((index > 1) & (index < SUBS + 2))
        def _():
            forward(1 - right, home, index - 2)

    wide = step // chunk * chunk
    tiles = [(lo, min(wide, heads * chunk - lo)) for lo in range(0, heads * chunk, wide)]

    def piece(part):
        cut = pl.ds(pl.multiple_of(part * chunk, chunk), chunk)
        def block(held, away, first):
            keys = jnp.concatenate([held[0], kext[away]], axis=1)
            values = jnp.concatenate([held[1, lo:lo + HD] for lo in range(0, rows, HD)], axis=1)
            if first:
                key = lax.broadcasted_iota(jnp.int32, (rows, chunk), 0)
                row = part * chunk + lax.broadcasted_iota(jnp.int32, (rows, chunk), 1)
                later = jnp.where(key <= row, 0.0, -1e30)
            def score(tile):
                lo, size = tile
                s = jnp.dot(keys, q_ref[part, :, lo:lo + size], preferred_element_type=jnp.float32)
                if first:
                    s = s + jnp.concatenate([later] * (size // chunk), axis=1)
                return s

            def weigh(tile, s):
                lo, size = tile
                fresh = jnp.max(s, axis=0, keepdims=True)
                scale = None
                if not first:
                    top = tops[:, lo:lo + size]
                    fresh = jnp.maximum(top, fresh)
                    scale = jnp.exp2(top - fresh)
                e = jnp.exp2(s - fresh)
                total = jnp.sum(e, axis=0, keepdims=True)
                if not first:
                    total = total + totals[:, lo:lo + size] * scale
                tops[:, lo:lo + size] = fresh
                totals[:, lo:lo + size] = total
                return tile, scale, e.astype(jnp.bfloat16)

            def mix(tile, scale, e):
                return tile, scale, jnp.dot(values, e, preferred_element_type=jnp.float32)

            def gather(tile, scale, pv):
                lo, size = tile
                if not first:
                    pv = pv + acc[:, lo:lo + size] * scale
                acc[:, lo:lo + size] = pv

            ready = [score(tile) for tile in tiles[:AHEAD]]
            mixed = []
            for index, tile in enumerate(tiles):
                if index + AHEAD < len(tiles):
                    ready.append(score(tiles[index + AHEAD]))
                mixed.append(mix(*weigh(tile, ready.pop(0))))
                if len(mixed) > BACK:
                    gather(*mixed.pop(0))
            while mixed:
                gather(*mixed.pop(0))

        @pl.when(part == 0)
        def _():
            bounce(0)

        block(kv_ref, 0, True)
        @pl.when(part == 0)
        def _():
            bounce(1)
            bounce(2)

        tail = (1 - core) * (behind // reach) * (reach % 2) if reach else 0

        @pl.loop(1, behind + 1)
        def _(turned):
            away = lax.rem(2 * behind - turned - tail + core, behind) + 1

            @pl.when(part == 0)
            def _():
                obtain(away)

            @pl.when((part == 0) & inner & (behind > 1) & (turned == behind))
            def _():
                offer()

            @pl.when((part == 1) & inner)
            def _():
                event(turned - 1)

            @pl.when((part == 1) & inner & (turned == behind - 1) & (behind > 4))
            def _():
                pass_straight()

            block(kv_in.at[away - 1], away, False)

        whole = acc[...] * (1.0 / totals[...])
        context = jnp.concatenate(
            [whole[:, h * chunk:(h + 1) * chunk].T.astype(jnp.bfloat16) for h in range(heads)], axis=1
        )
        ctx[cut, :] = context

        @pl.when((part == 1) & inner)
        def _():
            event(behind)

            @pl.when((behind > 1) & (behind < 5))
            def _():
                pass_straight()

        @pl.when(part == 0)
        def _():
            load.wait()

        def term(dest):
            sent[dest, cut] = jnp.dot(
                context, wo[:, pl.ds(pl.multiple_of(dest * cols, HD), cols)],
                preferred_element_type=jnp.float32,
            ).astype(jnp.bfloat16)

        def launch(dest):
            @pl.when((part == 0) & outer)
            def _():
                for index in range(SUBS):
                    term_copy(right, dest, index).start()

            @pl.when((part == 1) & outer)
            def _():
                for index in range(SUBS, TERMS):
                    term_copy(right, dest, index).start()

        term(far)
        launch(far)
        term(farther)
        launch(farther)

        @pl.when((part == 1) & outer)
        def _():
            for index in range(TERMS, 2 * SUBS):
                ctx_copy(index).start()
            for index in range(SUBS):
                term_copy(right, other, index).start()

        term(other)
        term(turn)

        @pl.when((part == 1) & outer)
        def _():
            for index in range(SUBS, TERMS):
                term_copy(right, other, index).start()

        @pl.when((part == 0) & inner & (behind < 2))
        def _():
            offer()

    @pl.loop(0, 2)
    def _(part):
        piece(part)

    @pl.when(inner)
    def _():
        split = jnp.where(behind > 1, behind + 1, 2 * SUBS - 1)
        early = (behind > 4) & (behind < 2 * SUBS - 2)

        @pl.loop(behind + 1, split)
        def _(index):
            event(index)

        @pl.when(behind < 2)
        def _():
            pass_straight()

        @pl.loop(split, 2 * SUBS)
        def _(index):
            event(index)

            @pl.when((index == 2 * SUBS - 2) & early)
            def _():
                hand_over(bent_steps)

        for index in range(SUBS, TERMS):
            forward(right, far, index)
            forward(right, farther, index)

        @pl.when(jnp.logical_not(early))
        def _():
            hand_over(bent_steps)

        twin = mine + 1 - 2 * lax.rem(mine, 2)
        for bits in [0] + steps:
            spread(mirror(twin, bits), 1, partner).wait_recv()

        @pl.loop(TERMS, 2 * SUBS)
        def _(index):
            cut = sub_cut(index)
            ctx_copy(index).wait_recv()
            guest = ctx_in[cut, :]
            for at in range(tp_count - 1):
                dest = at + 1 - right
                sent[dest, cut] = (
                    sent[dest, cut].astype(jnp.float32)
                    + jnp.dot(
                        guest, lent[:, at * cols:(at + 1) * cols], preferred_element_type=jnp.float32
                    )
                ).astype(jnp.bfloat16)
            term_copy(right, far, index).start()

        for index in range(TERMS, 2 * SUBS):
            term_copy(right, farther, index).start()
        for index in range(SUBS, 2 * SUBS):
            forward(1 - right, home, index)

    @pl.when(outer)
    def _():
        lend().wait_send()

    @pl.when(inner)
    def _():
        for copy in own_spreads() + [passed_spread(index) for index in range(len(steps))]:
            copy.wait_send()
        if bent_steps:
            cross().wait_send()

    each_send(lambda copy: copy.wait_send())
    each_relay(lambda copy: copy.wait_send())

    def finish(index):
        cut = sub_cut(index)
        term_wait(1 - right, turn, index)
        total = sent[turn, cut].astype(jnp.float32) + got[1 - right, turn, cut].astype(jnp.float32)
        both = inner & (index < TERMS)

        @pl.when(both)
        def _():
            term_wait(right, turn, index)
            out_ref[cut, :] = (total + got[right, turn, cut].astype(jnp.float32)).astype(jnp.bfloat16)

        @pl.when(jnp.logical_not(both))
        def _():
            out_ref[cut, :] = total.astype(jnp.bfloat16)

    @pl.loop(0, 2 * SUBS - 1)
    def _(index):
        finish(index)

    @pl.loop(0, 2 * SUBS)
    def _(index):
        @pl.when(inner | (index < TERMS))
        def _():
            for ahead in range(1, tp_count):
                term_copy(right, lax.rem(turn + ahead, tp_count), index).wait_send()

        @pl.when(outer & (index >= TERMS))
        def _():
            ctx_copy(index).wait_send()

    finish(2 * SUBS - 1)


def body(
    tokens, norm_gain, q_weight, q_bias, k_weight, k_bias, v_weight, v_bias, o_weight, doc_ids
):
    rows, model = tokens.shape
    seq_count = lax.axis_size("seq")
    tp_count = lax.axis_size("tp")
    width = q_weight.shape[1]
    cols = o_weight.shape[1] // tp_count
    reach = min(seq_count - 1, (seq_count * rows // 2 + 2 * rows - 2) // rows)
    chunk = rows // 2
    team = math.gcd(seq_count, 8)
    subs = rows // chunk * SUBS
    parts = rows // chunk
    near, far = rope_tables(rows, seq_count)
    hbm = pl.BlockSpec(memory_space=pltpu.HBM)
    vmem = pl.BlockSpec(memory_space=VMEM)
    slots = reach + 1
    spans = -(-width // (2 * HD))
    kdoc = doc_ids.reshape(seq_count, 1, rows)
    return pl.pallas_call(
        functools.partial(attend, seq_count, tp_count, reach, chunk, team),
        out_shape=jax.ShapeDtypeStruct((rows, cols), jnp.bfloat16),
        in_specs=[hbm] * 12,
        out_specs=vmem,
        scratch_shapes=[
            VMEM(norm_gain.shape, jnp.float32),
            VMEM(q_bias.shape, jnp.float32),
            VMEM(k_bias.shape, jnp.float32),
            VMEM(v_bias.shape, jnp.float32),
            VMEM(kdoc.shape, jnp.int32),
            VMEM(far.shape, jnp.float32),
            VMEM((rows, model), jnp.bfloat16),
            VMEM((rows, model), jnp.bfloat16),
            VMEM((model, width), jnp.bfloat16),
            VMEM((model, 2 * HD), jnp.bfloat16),
            VMEM(o_weight.shape, jnp.bfloat16),
            VMEM((2, rows, HD), jnp.float32),
            VMEM((parts, 2 * HD, width // HD * chunk), jnp.bfloat16),
            VMEM((2, rows, HD), jnp.bfloat16),
            VMEM((slots, 2, rows, HD), jnp.bfloat16),
            VMEM((slots, rows, HD), jnp.bfloat16),
            VMEM((HD, width // HD * chunk), jnp.float32),
            VMEM((1, width // HD * chunk), jnp.float32),
            VMEM((1, width // HD * chunk), jnp.float32),
            VMEM((rows, width), jnp.bfloat16),
            VMEM((rows, width), jnp.bfloat16),
            VMEM((width, (tp_count - 1) * cols), jnp.bfloat16),
            VMEM((tp_count, rows, cols), jnp.bfloat16),
            VMEM((2, tp_count, rows, cols), jnp.bfloat16),
            pltpu.SemaphoreType.DMA((14 + spans,)),
            pltpu.SemaphoreType.DMA((slots // 2 + 1, 3)),
            pltpu.SemaphoreType.DMA((max(slots // 2, 1), 3)),
            pltpu.SemaphoreType.DMA((slots, 3)),
            pltpu.SemaphoreType.DMA((3,)),
            pltpu.SemaphoreType.DMA((3,)),
            pltpu.SemaphoreType.DMA((tp_count - 1, subs)),
            pltpu.SemaphoreType.DMA(((tp_count - 1) * TERMS + 2 * subs,)),
            pltpu.SemaphoreType.DMA((subs - TERMS,)),
            pltpu.SemaphoreType.DMA((subs - TERMS,)),
            pltpu.SemaphoreType.DMA((team,)),
            pltpu.SemaphoreType.DMA((team,)),
        ],
        compiler_params=pltpu.CompilerParams(
            collective_id=0, has_side_effects=True, vmem_limit_bytes=52 * 1024 * 1024
        ),
    )(
        *[
            pltpu.with_memory_space_constraint(item, pltpu.HBM)
            for item in (
                tokens, norm_gain, q_weight, q_bias, k_weight, k_bias, v_weight, v_bias, o_weight,
                kdoc, jnp.asarray(near), jnp.asarray(far),
            )
        ]
    )


def solution(mesh):
    placed = (
        P("seq", None),
        P(),
        P(None, "tp"),
        P("tp"),
        P(None, "tp"),
        P("tp"),
        P(None, "tp"),
        P("tp"),
        P("tp", None),
        P(),
    )
    return jax.shard_map(
        body, mesh=mesh, in_specs=placed, out_specs=P("seq", "tp"), check_vma=False
    )
```
